32 devices in a mesh: dp: 8 (over z, y), group: 4 (over x, core).
Axes of the slice: x: 2, y: 2, z: 4, core: 2. Of those that a mesh axis runs over, the one named last changes fastest.
Arguments:
- deltas: bfloat16 [2048, 16, 4096], P(('dp', 'group')), may hold values from -96 to 96
- labels: int32 [2048, 1], P(('dp', 'group')), may hold values from 0 to 7; in each aligned block of 64 rows (0 to 63, 64 to 127, ...) at most 16 rows name the same one
Outputs:
- returned: bfloat16 [2048, 16, 4096], P(('dp', 'group'))
- cluster_rank: int32 [2048], P(('dp', 'group'))
The draws below stay inside these ranges and needn't reach their ends.
Inputs may be any that keep to these rules, and one draw needn't show every extreme that they name: `labels`: among the clients of one device at most 16 carry the same label, and that many do on some device; every cluster has at least one client.
All inputs are finite; a program needn't handle non-finite values.
Results may differ from the reference program's by a relative error of at most 0.0004.
Values may be sent and summed in bfloat16 or wider, within the bound.
No kernel may reach another device: no remote copies, remote signals or barrier semaphores. Data moves between devices by JAX's collectives and lax.ppermute only.
A program may use at most 128 MiB of HBM per device.

```python
import math
import jax
import jax.numpy as jnp
import numpy as np

BLOCK = 4096
CLUSTERS = 8
CAPACITY = 16
BLOCKS = 16
CL_DEV = 64
CLIENTS = 2048


def shard_levels(rng, extent, pieces, least, top_value):
    def one(position, shards_of):
        draws = jax.random.uniform(jax.random.fold_in(jax.random.fold_in(rng, 6), position), (shards_of,), jnp.float32, least / len(pieces), top_value / len(pieces))
        return jnp.repeat(jnp.exp(draws), extent[position] // shards_of).reshape((-1,) + (1,) * (len(extent) - position - 1))

    level = one(*pieces[0])
    for cut in pieces[1:]:
        level = level * one(*cut)
    return level


def routed_block(key, own, number, rows, count, top, limit, lean):
    sequence = jax.random.permutation(key, count)
    crowded, common = portions_of(count, rows * top, limit, lean, True), portions_of(count, rows * top, limit, lean, False)
    places = jnp.arange(count)

    def named(tallies, rotation):
        used = int((tallies > 0).sum())
        fixed = max(1, used // 4)
        passed = fixed + (places - fixed + rotation * (used - fixed)) % max(1, count - fixed)
        return jnp.zeros((count,), jnp.int32).at[sequence[jnp.where(places < fixed, places, passed)]].set(jnp.asarray(tallies, jnp.int32))

    tallies = jnp.where(number % 4 == 0, named(crowded, number // 4), named(common, number - number // 4 - 1))
    mixed = jax.random.permutation(jax.random.fold_in(own, 3), count)
    donor, taker = mixed[0:count // 2 * 2:2], mixed[1:count // 2 * 2:2]
    slack = jnp.minimum(tallies[donor] - 1, limit - tallies[taker]) // 2
    slack = jnp.where((donor == sequence[0]) | (taker == sequence[0]) | (tallies[taker] == 0), 0, jnp.maximum(slack, 0))
    passed = jax.random.randint(jax.random.fold_in(own, 4), (count // 2,), 0, 1 << 20) % (slack + 1)
    tallies = tallies.at[donor].add(-passed).at[taker].add(passed)
    members = jnp.searchsorted(jnp.cumsum(tallies), jnp.arange(rows * top), side="right").astype(jnp.int32)
    grid = members.reshape(top, rows).T
    grid = grid[jax.random.permutation(jax.random.fold_in(own, 1), rows)]
    rotation = jax.random.randint(jax.random.fold_in(own, 2), (rows, 1), 0, top)
    return jnp.take_along_axis(grid, (jnp.arange(top)[None, :] + rotation) % top, axis=1)


def portions_of(count, total, most, lean, full):
    portions = [(1 << 20) // math.isqrt(standing ** lean) + 1 for standing in range(1, count + 1)]
    largest = most if full else min(most, max(-(-total // count), total * portions[0] // sum(portions)))
    least = 1 if total - largest >= count - 1 else 0
    counts, rest = [largest] + [least] * (count - 1), total - largest - least * (count - 1)
    while rest > 0:
        movable = [i for i in range(1, count) if counts[i] < largest] or [i for i in range(1, count) if counts[i] < most]
        mass, budget = sum([portions[i] for i in movable]), rest
        for i in movable:
            extra = min(most - counts[i], max(1, budget * portions[i] // mass), rest)
            counts[i] = counts[i] + extra
            rest = rest - extra
    return np.array(counts)


def normal_values(key, shape, spread, most, shards=(), held_as=jnp.bfloat16):
    array = spread * jax.random.normal(key, shape, jnp.float32)
    if shards:
        array = array * shard_levels(key, shape, shards, -0.22, 0.18)
    return jnp.clip(array, -most, most).astype(held_as)


def setup_inputs(seed: int = 0) -> dict:
    arg_keys = jax.random.split(jax.random.key(seed), 3)
    deltas = normal_values(arg_keys[0], (CLIENTS, BLOCKS, BLOCK), 16.0, 96.0, ((0, 32),))
    labels_keys = jax.random.split(jax.random.fold_in(arg_keys[1], 1), CLIENTS // CL_DEV)
    labels_turns = jax.random.permutation(jax.random.fold_in(arg_keys[1], 3), CLIENTS // CL_DEV)
    labels = jax.vmap(lambda own, number: routed_block(jax.random.fold_in(arg_keys[1], 2), own, number, CL_DEV, CLUSTERS, 1, CAPACITY, 2))(labels_keys, labels_turns).reshape((CLIENTS, 1))
    return {"deltas": deltas, "labels": labels}


def reference(deltas, labels):
    flat = deltas.reshape(CLIENTS, BLOCKS * BLOCK)
    label_list = labels[:, 0]
    one_hot = (label_list[:, None] == jnp.arange(CLUSTERS, dtype=jnp.int32)[None, :]).astype(jnp.int32)
    before = jnp.cumsum(one_hot, axis=0) - one_hot
    cluster_rank = jnp.sum(before * one_hot, axis=1).astype(jnp.int32)
    totals = jnp.sum(one_hot, axis=0).astype(jnp.float32)
    sums = jnp.dot(one_hot.T.astype(jnp.bfloat16), flat, preferred_element_type=jnp.float32)
    models = (sums / totals[:, None]).astype(jnp.bfloat16)
    returned = jnp.dot(one_hot.astype(jnp.bfloat16), models, preferred_element_type=jnp.float32)
    returned = returned.astype(jnp.bfloat16).reshape(CLIENTS, BLOCKS, BLOCK)
    return returned, cluster_rank
```

```python
import functools

import jax
import jax.numpy as jnp
from jax import lax
from jax.experimental import pallas as pl
from jax.experimental.pallas import tpu as pltpu
from jax.sharding import PartitionSpec as P

CLUSTERS = 8
LANES = 128
AXES = ("dp", "group")
CHAINS = 2

VMEM = pl.BlockSpec(memory_space=pltpu.VMEM)
SMEM = pl.BlockSpec(memory_space=pltpu.SMEM)
ANY = pl.BlockSpec(memory_space=pl.ANY)


def count_rows(devices):
    return CLUSTERS * pl.cdiv(devices, LANES)


def local_sums_kernel(chain, devices, where, deltas, labels_row, other, mine, held, sems):
    clients, blocks, width = deltas.shape
    me = where[0]
    core = me & 1
    columns = width // CHAINS // 4
    copies = []
    for part in range(4):
        half = (1 - core) if part < 2 else core
        start = ((chain * 2 + half) * 2 + part % 2) * columns
        copies.append(pltpu.make_async_copy(
            deltas.at[:, :, pl.ds(pl.multiple_of(start, LANES), columns)], held.at[part], sems.at[part]))
        copies[-1].start()

    rows, depth = CLUSTERS * blocks, clients * blocks
    labels = labels_row[...]
    spread = (lax.broadcasted_iota(jnp.int32, (clients, depth), 1) // blocks
              == lax.broadcasted_iota(jnp.int32, (clients, depth), 0)).astype(jnp.bfloat16)
    wide = jnp.dot(jnp.broadcast_to(labels, (16, clients)).astype(jnp.bfloat16), spread,
                   preferred_element_type=jnp.float32)[0:1].astype(jnp.int32)
    row = lax.broadcasted_iota(jnp.int32, (rows, depth), 0)
    column = lax.broadcasted_iota(jnp.int32, (rows, depth), 1)
    pick = ((wide == row // blocks) & (column % blocks == row % blocks)).astype(jnp.bfloat16)

    hits = (labels == lax.broadcasted_iota(jnp.int32, (CLUSTERS, clients), 0)).astype(jnp.float32)
    counts = jnp.sum(hits, axis=1, keepdims=True)
    lane = lax.broadcasted_iota(jnp.int32, (CLUSTERS, LANES), 1)
    filled = 4 * (columns // 2) // LANES * rows
    for tile in range(count_rows(devices) // CLUSTERS):
        table = jnp.where(lane + tile * LANES == me, counts, 0.0)
        at = filled + tile * CLUSTERS
        other[at:at + CLUSTERS, :] = table
        mine[at:at + CLUSTERS, :] = table

    per_part = columns // LANES
    for part in range(4):
        copies[part].wait()
        sums = jnp.dot(pick, held[part].reshape(depth, columns), preferred_element_type=jnp.float32)
        target = other if part < 2 else mine
        for block in range(per_part):
            at = (part % 2 * per_part + block) * rows
            target[at:at + rows, :] = sums[:, block * LANES:(block + 1) * LANES]


def local_sums(chain, devices, where, deltas, labels_row):
    clients, blocks, width = deltas.shape
    columns = width // CHAINS // 4
    height = 2 * columns // LANES * CLUSTERS * blocks + count_rows(devices)
    out = jax.ShapeDtypeStruct((height, LANES), jnp.float32)
    return pl.pallas_call(
        functools.partial(local_sums_kernel, chain, devices),
        out_shape=(out, out),
        in_specs=[SMEM, ANY, VMEM],
        out_specs=(VMEM, VMEM),
        scratch_shapes=[pltpu.VMEM((4, clients, blocks, columns), jnp.bfloat16), pltpu.SemaphoreType.DMA((4,))],
        name="local_sums",
    )(where, deltas, labels_row)


def split_kernel(tail, pick, kept, arrived, send, keep):
    half = (kept.shape[0] - tail) // 2
    bit = pick[0]
    for target, which in ((send, 1 - bit), (keep, bit)):
        rows = pl.ds(pl.multiple_of(which * half, CLUSTERS), half)
        target[0:half, :] = kept[rows, :] + arrived[rows, :]
        target[half:half + tail, :] = kept[2 * half:2 * half + tail, :] + arrived[2 * half:2 * half + tail, :]


def split(tail, bit, kept, arrived):
    half = (kept.shape[0] - tail) // 2
    out = jax.ShapeDtypeStruct((half + tail, LANES), jnp.float32)
    return pl.pallas_call(
        functools.partial(split_kernel, tail),
        out_shape=(out, out),
        in_specs=[SMEM, VMEM, VMEM],
        out_specs=(VMEM, VMEM),
        name="split",
    )(bit, kept, arrived)


def finish_kernel(tail, blocks, kept, arrived, models):
    rows = CLUSTERS * blocks
    height = kept.shape[0] - tail
    totals = jnp.zeros((CLUSTERS, 1), jnp.float32)
    for at in range(height, height + tail, CLUSTERS):
        table = kept[at:at + CLUSTERS, :] + arrived[at:at + CLUSTERS, :]
        totals = totals + jnp.sum(table, axis=1, keepdims=True)
    for cluster in range(CLUSTERS):
        total = jnp.broadcast_to(totals[cluster:cluster + 1, :], (blocks, LANES))
        for block in range(height // rows):
            at = block * rows + cluster * blocks
            sums = kept[at:at + blocks, :] + arrived[at:at + blocks, :]
            models[cluster * blocks:(cluster + 1) * blocks, block * LANES:(block + 1) * LANES] = (
                sums / total).astype(jnp.bfloat16)


def finish(tail, blocks, kept, arrived):
    rows = CLUSTERS * blocks
    columns = (kept.shape[0] - tail) // rows * LANES
    return pl.pallas_call(
        functools.partial(finish_kernel, tail, blocks),
        out_shape=jax.ShapeDtypeStruct((rows, columns), jnp.bfloat16),
        in_specs=[VMEM, VMEM],
        out_specs=VMEM,
        name="finish",
    )(kept, arrived)


def rank_kernel(tail, where, kept, arrived, labels_row, labels_column, rank):
    height = kept.shape[0] - tail
    clients = labels_row.shape[1]
    lane = lax.broadcasted_iota(jnp.int32, (CLUSTERS, LANES), 1)
    before = jnp.zeros((CLUSTERS, 1), jnp.float32)
    for tile in range(tail // CLUSTERS):
        at = height + tile * CLUSTERS
        table = kept[at:at + CLUSTERS, :] + arrived[at:at + CLUSTERS, :]
        before = before + jnp.sum(jnp.where(lane + tile * LANES < where[0], table, 0.0), axis=1, keepdims=True)
    labels = labels_row[...]
    hits = labels == lax.broadcasted_iota(jnp.int32, (CLUSTERS, clients), 0)
    offset = jnp.sum(jnp.where(hits, before, 0.0), axis=0, keepdims=True)
    earlier = (lax.broadcasted_iota(jnp.int32, (clients, clients), 0)
               < lax.broadcasted_iota(jnp.int32, (clients, clients), 1))
    local = jnp.sum(jnp.where((labels_column[...] == labels) & earlier, 1.0, 0.0), axis=0, keepdims=True)
    rank[...] = (offset + local).astype(jnp.int32)


def ranks(tail, where, kept, arrived, labels_row, labels_column):
    return pl.pallas_call(
        functools.partial(rank_kernel, tail),
        out_shape=jax.ShapeDtypeStruct(labels_row.shape, jnp.int32),
        in_specs=[SMEM, VMEM, VMEM, VMEM, VMEM],
        out_specs=VMEM,
        name="ranks",
    )(where, kept, arrived, labels_row, labels_column)


def return_kernel(pick, labels, models, *rest):
    returned, laid, sem = rest[-3:]
    pieces, rows, columns = models.shape
    clients, blocks, _ = returned.shape
    for piece in range(pieces):
        slot = piece ^ pick[1]
        for cluster in range(CLUSTERS):
            laid[cluster, :, piece * columns:(piece + 1) * columns] = models[
                slot, cluster * blocks:(cluster + 1) * blocks, :]
    start = pl.multiple_of(pick[0] * (pieces * columns), LANES)

    def copy(client):
        return pltpu.make_async_copy(
            laid.at[labels[client]], returned.at[client, :, pl.ds(start, pieces * columns)], sem)

    for client in range(clients):
        copy(client).start()
    for client in range(clients):
        copy(client).wait()


def give_back(pick, labels, models, shape, returned):
    pieces, rows, columns = models.shape
    blocks = shape[1]
    given = () if returned is None else (returned,)
    return pl.pallas_call(
        return_kernel,
        out_shape=jax.ShapeDtypeStruct(shape, jnp.bfloat16),
        in_specs=[SMEM, SMEM, VMEM] + [ANY] * len(given),
        out_specs=ANY,
        scratch_shapes=[pltpu.VMEM((CLUSTERS, blocks, pieces * columns), jnp.bfloat16), pltpu.SemaphoreType.DMA],
        input_output_aliases={3: 0} if given else {},
        name="give_back",
    )(pick, labels, models, *given)


def on_device(devices, deltas, labels):
    clients, blocks, width = deltas.shape
    me = lax.axis_index(AXES).astype(jnp.int32)
    where = me.reshape(1)
    labels_row = labels.reshape(1, clients)
    labels_list = labels.reshape(clients)
    tail = count_rows(devices)
    bits = devices.bit_length() - 1
    core = me & 1

    def send(value, flip):
        return lax.ppermute(value, AXES, [(i, i ^ flip(i)) for i in range(devices)])

    def order(chain, low, high):
        def at(step):
            def flip(i):
                taken = list(range(low, high))
                if (i & 1) ^ chain:
                    taken = taken[::-1]
                return 1 << taken[step]
            return flip
        return at

    def bit_at(core, chain, step):
        return (me >> (1 + (core ^ chain ^ step))) & 1

    state = []
    for chain in range(CHAINS):
        state.append(local_sums(chain, devices, where, deltas, labels_row))
    returned, rank = None, None
    kept = [None] * CHAINS
    for chain in range(CHAINS):
        other, mine = state[chain]
        arrived = send(other, lambda i: 1)
        kept[chain] = split(tail, bit_at(core, chain, 0).reshape(1), mine, arrived)
    scatter = [order(chain, 1, 3) for chain in range(CHAINS)]
    reduce = [order(chain, 3, bits) for chain in range(CHAINS)]
    for chain in range(CHAINS):
        out, keep = kept[chain]
        kept[chain] = split(tail, bit_at(core, chain, 1).reshape(1), keep, send(out, scatter[chain](0)))
    for chain in range(CHAINS):
        out, keep = kept[chain]
        kept[chain] = (keep, send(out, scatter[chain](1)))
    for step in range(bits - 3):
        for chain in range(CHAINS):
            keep, arrived = kept[chain]
            total = keep + arrived
            kept[chain] = (total, send(total, reduce[chain](step)))
    rank = ranks(tail, where, *kept[0], labels_row, labels)
    models = [finish(tail, blocks, *kept[chain])[None] for chain in range(CHAINS)]
    for step in (1, 0):
        for chain in range(CHAINS):
            own = models[chain]
            models[chain] = jnp.concatenate([own, send(own, scatter[chain](step))], axis=0)
    for chain in range(CHAINS):
        arrived = send(models[chain], lambda i: 1)
        for half, value in ((core, models[chain]), (1 - core, arrived)):
            mask = bit_at(half, chain, 0) * 2 + bit_at(half, chain, 1)
            pick = jnp.stack([chain * 2 + half, mask])
            returned = give_back(pick, labels_list, value, deltas.shape, returned)
    return returned, rank.reshape(clients)


def solution(mesh):
    devices = mesh.shape["dp"] * mesh.shape["group"]
    placed = (P(AXES, None, None), P(AXES, None))
    return jax.shard_map(
        functools.partial(on_device, devices),
        mesh=mesh,
        in_specs=placed,
        out_specs=(P(AXES, None, None), P(AXES)),
        check_vma=False,
    )
```

```python
import functools

import jax
import jax.numpy as jnp
from jax import lax
from jax.experimental import pallas as pl
from jax.experimental.pallas import tpu as pltpu
from jax.sharding import PartitionSpec as P


CLUSTERS = 8
LANES = 128
AXES = ("dp", "group")
SHARES = (2, 2)
COVER = 1 << 26

VMEM = pl.BlockSpec(memory_space=pltpu.VMEM)
SMEM = pl.BlockSpec(memory_space=pltpu.SMEM)
ANY = pl.BlockSpec(memory_space=pl.ANY)


def shares_of(width):
    unit = width // (8 * sum(SHARES))
    starts = [8 * unit * sum(SHARES[:at]) for at in range(len(SHARES))]
    return [(start, unit * share) for start, share in zip(starts, SHARES)]


def near(value):
    return pltpu.with_memory_space_constraint(value, pltpu.VMEM)


def count_rows(devices):
    return CLUSTERS * pl.cdiv(devices, LANES)


def local_sums_kernel(devices, where, deltas, labels_row, *rest):
    chains = len(SHARES)
    targets, helds, sems = rest[:2 * chains], rest[2 * chains:3 * chains], rest[-1]
    clients, blocks, width = deltas.shape
    me = where[0]
    core = me & 1
    work = []
    for chain, (first, columns) in enumerate(shares_of(width)):
        for part in range(4):
            half = (1 - core) if part < 2 else core
            start = pl.multiple_of(first + (half * 2 + part % 2) * 2 * columns, LANES)
            copy = pltpu.make_async_copy(
                deltas.at[:, :, pl.ds(start, 2 * columns)], helds[chain].at[part], sems.at[chain, part])
            copy.start()
            work.append((copy, helds[chain].at[part], targets[2 * chain + part // 2], part % 2))

    rows, depth = CLUSTERS * blocks, clients * blocks
    labels = labels_row[...]
    spread = (lax.broadcasted_iota(jnp.int32, (clients, depth), 1) // blocks
              == lax.broadcasted_iota(jnp.int32, (clients, depth), 0)).astype(jnp.bfloat16)
    wide = jnp.dot(jnp.broadcast_to(labels, (16, clients)).astype(jnp.bfloat16), spread,
                   preferred_element_type=jnp.float32)[0:1].astype(jnp.int32)
    row = lax.broadcasted_iota(jnp.int32, (rows, depth), 0)
    column = lax.broadcasted_iota(jnp.int32, (rows, depth), 1)
    pick = ((wide == row // blocks) & (column % blocks == row % blocks)).astype(jnp.bfloat16)

    hits = (labels == lax.broadcasted_iota(jnp.int32, (CLUSTERS, clients), 0)).astype(jnp.float32)
    counts = jnp.sum(hits, axis=1, keepdims=True)
    lane = lax.broadcasted_iota(jnp.int32, (CLUSTERS, LANES), 1)
    tail = count_rows(devices)
    for tile in range(tail // CLUSTERS):
        table = jnp.where(lane + tile * LANES == me, counts, 0.0)
        for target in targets:
            at = target.shape[0] - tail + tile * CLUSTERS
            target[at:at + CLUSTERS, :] = table

    for copy, held, target, part in work:
        copy.wait()
        columns = held.shape[2]
        sums = jnp.dot(pick, held[...].reshape(depth, columns), preferred_element_type=jnp.float32)
        for block in range(columns // LANES):
            to = (part * columns // LANES + block) * rows
            target[to:to + rows, :] = sums[:, block * LANES:(block + 1) * LANES]


def local_sums(devices, where, deltas, labels_row):
    clients, blocks, width = deltas.shape
    outs, helds = [], []
    for _, columns in shares_of(width):
        height = 4 * columns // LANES * CLUSTERS * blocks + count_rows(devices)
        outs += [pltpu.VMEM((height, LANES), jnp.float32)] * 2
        helds.append(pltpu.VMEM((4, clients, blocks, 2 * columns), jnp.bfloat16))
    sums = pl.pallas_call(
        functools.partial(local_sums_kernel, devices),
        out_shape=outs,
        in_specs=[SMEM, pl.BlockSpec(memory_space=pltpu.HBM), VMEM],
        out_specs=[VMEM] * len(outs),
        scratch_shapes=helds + [pltpu.SemaphoreType.DMA((len(SHARES), 4))],
        compiler_params=pltpu.CompilerParams(vmem_limit_bytes=24 << 20),
        name="local_sums",
    )(where, pltpu.with_memory_space_constraint(deltas, pltpu.HBM), labels_row)
    return list(zip(sums[::2], sums[1::2]))


def bit_at(me, core, step):
    return (me >> (1 + (core ^ step))) & 1


def split_kernel(tail, step, where, kept, arrived, send, keep):
    half = (kept.shape[0] - tail) // 2
    bit = bit_at(where[0], where[0] & 1, step)
    for target, which in ((send, 1 - bit), (keep, bit)):
        rows = pl.ds(pl.multiple_of(which * half, CLUSTERS), half)
        target[0:half, :] = kept[rows, :] + arrived[rows, :]
        target[half:half + tail, :] = kept[2 * half:2 * half + tail, :] + arrived[2 * half:2 * half + tail, :]


def split(tail, step, where, kept, arrived):
    half = (kept.shape[0] - tail) // 2
    out = pltpu.VMEM((half + tail, LANES), jnp.float32)
    return pl.pallas_call(
        functools.partial(split_kernel, tail, step),
        out_shape=(out, out),
        in_specs=[SMEM, VMEM, VMEM],
        out_specs=(VMEM, VMEM),
        compiler_params=pltpu.CompilerParams(vmem_limit_bytes=8 << 20),
        name="split",
    )(where, near(kept), near(arrived))


def table_of(tail, kept, arrived):
    ends = [kept.shape[0] - tail + at for at in range(0, tail, CLUSTERS)]
    return [kept[at:at + CLUSTERS, :] + arrived[at:at + CLUSTERS, :] for at in ends]


def finish_kernel(tail, blocks, kept, arrived, models):
    rows = CLUSTERS * blocks
    height = kept.shape[0] - tail
    totals = jnp.zeros((CLUSTERS, 1), jnp.float32)
    for counts in table_of(tail, kept, arrived):
        totals = totals + jnp.sum(counts, axis=1, keepdims=True)
    for cluster in range(CLUSTERS):
        total = jnp.broadcast_to(totals[cluster:cluster + 1, :], (blocks, LANES))
        for block in range(height // rows):
            at = block * rows + cluster * blocks
            sums = kept[at:at + blocks, :] + arrived[at:at + blocks, :]
            models[cluster * blocks:(cluster + 1) * blocks, block * LANES:(block + 1) * LANES] = (
                sums / total).astype(jnp.bfloat16)


def finish(tail, blocks, kept, arrived):
    rows = CLUSTERS * blocks
    columns = (kept.shape[0] - tail) // rows * LANES
    return pl.pallas_call(
        functools.partial(finish_kernel, tail, blocks),
        out_shape=pltpu.VMEM((rows, columns), jnp.bfloat16),
        in_specs=[VMEM, VMEM],
        out_specs=VMEM,
        compiler_params=pltpu.CompilerParams(vmem_limit_bytes=8 << 20),
        name="finish",
    )(near(kept), near(arrived))


def ranks_of(me, table, labels):
    clients = labels.shape[1]
    lane = lax.broadcasted_iota(jnp.int32, (CLUSTERS, LANES), 1)
    before = jnp.zeros((CLUSTERS, 1), jnp.float32)
    for tile, counts in enumerate(table):
        before = before + jnp.sum(jnp.where(lane + tile * LANES < me, counts, 0.0), axis=1, keepdims=True)
    hits = labels == lax.broadcasted_iota(jnp.int32, (CLUSTERS, clients), 0)
    earlier = (lax.broadcasted_iota(jnp.int32, (clients, clients), 0)
               < lax.broadcasted_iota(jnp.int32, (clients, clients), 1))
    local = jnp.dot(hits.astype(jnp.float32).astype(jnp.bfloat16), earlier.astype(jnp.float32).astype(jnp.bfloat16),
                    preferred_element_type=jnp.float32)
    return jnp.sum(jnp.where(hits, before + local, 0.0), axis=0, keepdims=True).astype(jnp.int32)


def give_back_kernel(first, tail, where, labels, near_by, taken, far, *rest):
    me = where[0]
    if tail:
        kept, arrived, labels_row, returned, rank, laid, sem = rest
    else:
        _, returned, laid, sem = rest
    _, _, columns = near_by.shape
    clients, blocks, _ = returned.shape
    core = me & 1
    beside, opposite = 2 << core, 4 >> core
    for source, slot, half, flip in (
            (near_by, 0, core, 0), (near_by, 1, 1 - core, 0), (taken, 0, core, 6), (taken, 1, core, beside),
            (taken, 2, 1 - core, beside), (far, 0, 1 - core, 6), (far, 1, 1 - core, opposite),
            (far, 2, core, opposite)):
        owner = me ^ flip
        piece = half * 4 + bit_at(owner, half, 0) * 2 + bit_at(owner, half, 1)
        to = pl.ds(pl.multiple_of(piece * columns, LANES), columns)
        for cluster in range(CLUSTERS):
            laid[cluster, :, to] = source[slot, cluster * blocks:(cluster + 1) * blocks, :]
    across = pl.ds(first, 8 * columns)
    for client in range(clients):
        pltpu.make_async_copy(laid.at[labels[client]], returned.at[client, :, across], sem).start()
    if tail:
        rank[...] = ranks_of(me, table_of(tail, kept, arrived), labels_row[...])
    whole = returned.at[:, :, across]
    pltpu.make_async_copy(whole, whole, sem).wait()


def give_back(first, where, labels, values, shape, returned=None, ranked=None):
    columns = values[0].shape[2]
    blocks = shape[1]
    out = [jax.ShapeDtypeStruct(shape, jnp.bfloat16)]
    if ranked is None:
        tail, more, more_specs, aliases = 0, (returned,), [ANY], {2 + len(values): 0}
    else:
        tail, kept, arrived, labels_row = ranked
        more, more_specs, aliases = (near(kept), near(arrived), labels_row), [VMEM] * 3, {}
        out.append(jax.ShapeDtypeStruct(labels_row.shape, jnp.int32))
    return pl.pallas_call(
        functools.partial(give_back_kernel, first, tail),
        out_shape=out,
        in_specs=[SMEM, SMEM] + [VMEM] * len(values) + more_specs,
        out_specs=[ANY, VMEM][:len(out)],
        scratch_shapes=[pltpu.VMEM((CLUSTERS, blocks, 8 * columns), jnp.bfloat16), pltpu.SemaphoreType.DMA],
        input_output_aliases=aliases,
        compiler_params=pltpu.CompilerParams(vmem_limit_bytes=8 << 20),
        cost_estimate=pl.CostEstimate(flops=COVER, bytes_accessed=0, transcendentals=0),
        name="give_back",
    )(where, labels, *[near(value) for value in values], *more)


def on_device(devices, deltas, labels):
    clients, blocks, width = deltas.shape
    where = lax.axis_index(AXES).astype(jnp.int32).reshape(1)
    labels_row = labels.reshape(1, clients)
    labels_list = labels.reshape(clients)
    tail = count_rows(devices)
    bits = devices.bit_length() - 1

    def send(value, flip):
        return lax.ppermute(value, AXES, [(i, i ^ flip(i)) for i in range(devices)])

    def cores(i):
        return 1

    def crossed(low, high, step):
        def flip(i):
            return 1 << (high - 1 - step if i & 1 else low + step)

        return flip

    kept = []
    for other, mine in local_sums(devices, where, deltas, labels_row):
        kept.append(split(tail, 0, where, mine, send(other, cores)))
    for chain, (out, keep) in enumerate(kept):
        kept[chain] = split(tail, 1, where, keep, send(out, crossed(1, 3, 0)))
    for chain, (out, keep) in enumerate(kept):
        kept[chain] = (keep, send(out, crossed(1, 3, 1)))
    for step in range(bits - 3):
        for chain, (keep, arrived) in enumerate(kept):
            total = keep + arrived
            kept[chain] = (total, send(total, crossed(3, bits, step)))
    values = []
    for pair in kept:
        own = finish(tail, blocks, *pair)[None]
        near_by = jnp.concatenate([own, send(own, cores)], axis=0)
        diagonal = send(own, lambda i: 6)
        beside = send(near_by, lambda i: 2 << (i & 1))
        taken = jnp.concatenate([diagonal, beside], axis=0)
        values.append((near_by, taken, send(taken, cores)))

    give = functools.partial(give_back, where=where, labels=labels_list, shape=deltas.shape)
    starts = [first for first, _ in shares_of(width)]
    returned, rank = give(starts[0], values=values[0], ranked=(tail, *kept[0], labels_row))
    for chain in range(1, len(SHARES)):
        returned, = give(starts[chain], values=values[chain], returned=returned)
    return returned, rank.reshape(clients)


def solution(mesh):
    devices = mesh.shape["dp"] * mesh.shape["group"]
    placed = (P(AXES, None, None), P(AXES, None))

    def body(deltas, labels):
        return on_device(devices, deltas, labels)

    return jax.shard_map(
        body,
        mesh=mesh,
        in_specs=placed,
        out_specs=(P(AXES, None, None), P(AXES)),
        check_vma=False,
    )
```

```python
import functools

import jax
import jax.numpy as jnp
from jax import lax
from jax.experimental import pallas as pl
from jax.experimental.pallas import tpu as pltpu
from jax.sharding import PartitionSpec as P


CLUSTERS = 8
LANES = 128
AXES = ("dp", "group")
SHARES = (2, 2)
COVER = 1 << 26

VMEM = pl.BlockSpec(memory_space=pltpu.VMEM)
SMEM = pl.BlockSpec(memory_space=pltpu.SMEM)
ANY = pl.BlockSpec(memory_space=pl.ANY)
HBM = pl.BlockSpec(memory_space=pltpu.HBM)


def shares_of(width):
    unit = width // (8 * sum(SHARES))
    starts = [8 * unit * sum(SHARES[:at]) for at in range(len(SHARES))]
    return [(start, unit * share) for start, share in zip(starts, SHARES)]


def role_of(index):
    for shift in (16, 8, 4, 2, 1):
        index = index ^ (index >> shift)
    return index & 1


def near(value):
    return pltpu.with_memory_space_constraint(value, pltpu.VMEM)


def far_off(value):
    return pltpu.with_memory_space_constraint(value, pltpu.HBM)


def count_rows(devices):
    return CLUSTERS * pl.cdiv(devices, LANES)


def local_sums_kernel(devices, first, where, deltas, labels_row, other, mine, held, labels_here, sems):
    clients, blocks, _ = deltas.shape
    me = where[0]
    role = role_of(me)
    columns = held.shape[3]
    arrive = pltpu.make_async_copy(labels_row, labels_here, sems.at[4])
    arrive.start()
    copies = []
    for part in range(4):
        half = (1 - role) if part < 2 else role
        start = pl.multiple_of(first + (half * 2 + part % 2) * columns, LANES)
        copies.append(pltpu.make_async_copy(deltas.at[:, :, pl.ds(start, columns)], held.at[part], sems.at[part]))
        copies[-1].start()

    rows, depth = CLUSTERS * blocks, clients * blocks
    spread = (lax.broadcasted_iota(jnp.int32, (clients, depth), 1) // blocks
              == lax.broadcasted_iota(jnp.int32, (clients, depth), 0)).astype(jnp.bfloat16)
    row = lax.broadcasted_iota(jnp.int32, (rows, depth), 0)
    column = lax.broadcasted_iota(jnp.int32, (rows, depth), 1)
    same_row = column % blocks == row % blocks
    arrive.wait()
    labels = labels_here[...]
    wide = jnp.dot(jnp.broadcast_to(labels, (16, clients)).astype(jnp.bfloat16), spread,
                   preferred_element_type=jnp.float32)[0:1].astype(jnp.int32)
    pick = ((wide == row // blocks) & same_row).astype(jnp.bfloat16)

    hits = (labels == lax.broadcasted_iota(jnp.int32, (CLUSTERS, clients), 0)).astype(jnp.float32)
    counts = jnp.sum(hits, axis=1, keepdims=True)
    lane = lax.broadcasted_iota(jnp.int32, (CLUSTERS, LANES), 1)
    tail = count_rows(devices)
    for tile in range(tail // CLUSTERS):
        table = jnp.where(lane + tile * LANES == me, counts, 0.0)
        at = other.shape[0] - tail + tile * CLUSTERS
        other[at:at + CLUSTERS, :] = table
        mine[at:at + CLUSTERS, :] = table

    for part in range(4):
        copies[part].wait()
        sums = jnp.dot(pick, held[part].reshape(depth, columns), preferred_element_type=jnp.float32)
        target = other if part < 2 else mine
        for block in range(columns // LANES):
            to = (part % 2 * columns // LANES + block) * rows
            target[to:to + rows, :] = sums[:, block * LANES:(block + 1) * LANES]


def local_sums(devices, first, columns, where, deltas, labels_row):
    clients, blocks, _ = deltas.shape
    height = 4 * columns // LANES * CLUSTERS * blocks + count_rows(devices)
    out = pltpu.VMEM((height, LANES), jnp.float32)
    return pl.pallas_call(
        functools.partial(local_sums_kernel, devices, first),
        out_shape=(out, out),
        in_specs=[SMEM, HBM, HBM],
        out_specs=(VMEM, VMEM),
        scratch_shapes=[
            pltpu.VMEM((4, clients, blocks, 2 * columns), jnp.bfloat16), pltpu.VMEM((1, clients), jnp.int32),
            pltpu.SemaphoreType.DMA((5,))],
        compiler_params=pltpu.CompilerParams(vmem_limit_bytes=16 << 20),
        name="local_sums",
    )(where, far_off(deltas), far_off(labels_row))


def bit_at(me, role, step):
    return (me >> (1 + (role ^ step))) & 1


def split_kernel(tail, step, where, kept, arrived, send, keep):
    half = (kept.shape[0] - tail) // 2
    bit = bit_at(where[0], role_of(where[0]), step)
    for target, which in ((send, 1 - bit), (keep, bit)):
        rows = pl.ds(pl.multiple_of(which * half, CLUSTERS), half)
        target[0:half, :] = kept[rows, :] + arrived[rows, :]
        target[half:half + tail, :] = kept[2 * half:2 * half + tail, :] + arrived[2 * half:2 * half + tail, :]


def split(tail, step, where, kept, arrived):
    half = (kept.shape[0] - tail) // 2
    out = pltpu.VMEM((half + tail, LANES), jnp.float32)
    return pl.pallas_call(
        functools.partial(split_kernel, tail, step),
        out_shape=(out, out),
        in_specs=[SMEM, VMEM, VMEM],
        out_specs=(VMEM, VMEM),
        compiler_params=pltpu.CompilerParams(vmem_limit_bytes=8 << 20),
        name="split",
    )(where, near(kept), near(arrived))


def table_of(tail, kept, arrived):
    ends = [kept.shape[0] - tail + at for at in range(0, tail, CLUSTERS)]
    return [kept[at:at + CLUSTERS, :] + arrived[at:at + CLUSTERS, :] for at in ends]


def finish_kernel(tail, blocks, kept, arrived, models):
    rows = CLUSTERS * blocks
    height = kept.shape[0] - tail
    totals = jnp.zeros((CLUSTERS, 1), jnp.float32)
    for counts in table_of(tail, kept, arrived):
        totals = totals + jnp.sum(counts, axis=1, keepdims=True)
    for cluster in range(CLUSTERS):
        total = jnp.broadcast_to(totals[cluster:cluster + 1, :], (blocks, LANES))
        for block in range(height // rows):
            at = block * rows + cluster * blocks
            sums = kept[at:at + blocks, :] + arrived[at:at + blocks, :]
            models[cluster * blocks:(cluster + 1) * blocks, block * LANES:(block + 1) * LANES] = (
                sums / total).astype(jnp.bfloat16)


def finish(tail, blocks, kept, arrived):
    rows = CLUSTERS * blocks
    columns = (kept.shape[0] - tail) // rows * LANES
    return pl.pallas_call(
        functools.partial(finish_kernel, tail, blocks),
        out_shape=pltpu.VMEM((rows, columns), jnp.bfloat16),
        in_specs=[VMEM, VMEM],
        out_specs=VMEM,
        compiler_params=pltpu.CompilerParams(vmem_limit_bytes=8 << 20),
        name="finish",
    )(near(kept), near(arrived))


def ranks_of(me, table, labels):
    clients = labels.shape[1]
    lane = lax.broadcasted_iota(jnp.int32, (CLUSTERS, LANES), 1)
    before = jnp.zeros((CLUSTERS, 1), jnp.float32)
    for tile, counts in enumerate(table):
        before = before + jnp.sum(jnp.where(lane + tile * LANES < me, counts, 0.0), axis=1, keepdims=True)
    hits = labels == lax.broadcasted_iota(jnp.int32, (CLUSTERS, clients), 0)
    earlier = (lax.broadcasted_iota(jnp.int32, (clients, clients), 0)
               < lax.broadcasted_iota(jnp.int32, (clients, clients), 1))
    local = jnp.dot(hits.astype(jnp.float32).astype(jnp.bfloat16), earlier.astype(jnp.float32).astype(jnp.bfloat16),
                    preferred_element_type=jnp.float32)
    return jnp.sum(jnp.where(hits, before + local, 0.0), axis=0, keepdims=True).astype(jnp.int32)


def give_back_kernel(first, tail, where, labels, near_by, taken, far, *rest):
    me = where[0]
    if tail:
        kept, arrived, labels_row, returned, rank, laid, sem, rank_here, rank_sem = rest
    else:
        _, returned, laid, sem = rest
    _, _, columns = near_by.shape
    clients, blocks, _ = returned.shape
    role = role_of(me)
    beside, opposite = 2 << role, 4 >> role
    for source, slot, half, flip in (
            (near_by, 0, role, 0), (near_by, 1, 1 - role, 0), (taken, 0, role, 6), (taken, 1, role, beside),
            (taken, 2, 1 - role, beside), (far, 0, 1 - role, 6), (far, 1, 1 - role, opposite),
            (far, 2, role, opposite)):
        owner = me ^ flip
        piece = half * 4 + bit_at(owner, half, 0) * 2 + bit_at(owner, half, 1)
        to = pl.ds(pl.multiple_of(piece * columns, LANES), columns)
        for cluster in range(CLUSTERS):
            laid[cluster, :, to] = source[slot, cluster * blocks:(cluster + 1) * blocks, :]
    across = pl.ds(first, 8 * columns)
    for client in range(clients):
        pltpu.make_async_copy(laid.at[labels[client]], returned.at[client, :, across], sem).start()
    if tail:
        rank_here[...] = ranks_of(me, table_of(tail, kept, arrived), labels_row[...])
        ranks = pltpu.make_async_copy(rank_here, rank, rank_sem)
        ranks.start()
        ranks.wait()
    whole = returned.at[:, :, across]
    pltpu.make_async_copy(whole, whole, sem).wait()


def give_back(first, where, labels, values, shape, returned=None, ranked=None):
    columns = values[0].shape[2]
    blocks = shape[1]
    scratch = [pltpu.VMEM((CLUSTERS, blocks, 8 * columns), jnp.bfloat16), pltpu.SemaphoreType.DMA]
    out = [jax.ShapeDtypeStruct(shape, jnp.bfloat16)]
    if ranked is None:
        tail, more, more_specs, aliases = 0, (returned,), [ANY], {2 + len(values): 0}
    else:
        tail, kept, arrived, labels_row = ranked
        more, more_specs, aliases = (near(kept), near(arrived), near(labels_row)), [VMEM] * 3, {}
        out.append(jax.ShapeDtypeStruct(labels_row.shape, jnp.int32))
        scratch += [pltpu.VMEM(labels_row.shape, jnp.int32), pltpu.SemaphoreType.DMA]
    return pl.pallas_call(
        functools.partial(give_back_kernel, first, tail),
        out_shape=out,
        in_specs=[SMEM, SMEM] + [VMEM] * len(values) + more_specs,
        out_specs=[ANY] * len(out),
        scratch_shapes=scratch,
        input_output_aliases=aliases,
        compiler_params=pltpu.CompilerParams(vmem_limit_bytes=8 << 20),
        cost_estimate=pl.CostEstimate(flops=COVER, bytes_accessed=0, transcendentals=0),
        name="give_back",
    )(where, labels, *[near(value) for value in values], *more)


def on_device(devices, deltas, labels):
    clients, blocks, width = deltas.shape
    where = lax.axis_index(AXES).astype(jnp.int32).reshape(1)
    labels_row = labels.reshape(1, clients)
    labels_list = labels.reshape(clients)
    tail = count_rows(devices)
    bits = devices.bit_length() - 1

    def send(value, flip):
        return lax.ppermute(value, AXES, [(i, i ^ flip(i)) for i in range(devices)])

    def cores(i):
        return 1

    def crossed(low, high, step):
        def flip(i):
            return 1 << (high - 1 - step if role_of(i) else low + step) | 1

        return flip

    kept = []
    for first, columns in shares_of(width):
        other, mine = local_sums(devices, first, columns, where, deltas, labels_row)
        kept.append(split(tail, 0, where, mine, send(other, cores)))
    for chain, (out, keep) in enumerate(kept):
        kept[chain] = split(tail, 1, where, keep, send(out, crossed(1, 3, 0)))
    for chain, (out, keep) in enumerate(kept):
        kept[chain] = (keep, send(out, crossed(1, 3, 1)))
    for step in range(bits - 3):
        for chain, (keep, arrived) in enumerate(kept):
            total = keep + arrived
            kept[chain] = (total, send(total, crossed(3, bits, step)))
    values = []
    for pair in kept:
        own = finish(tail, blocks, *pair)[None]
        near_by = jnp.concatenate([own, send(own, cores)], axis=0)
        diagonal = send(own, lambda i: 6)
        beside = send(near_by, lambda i: 2 << role_of(i) | 1)
        taken = jnp.concatenate([diagonal, beside], axis=0)
        values.append((near_by, taken, send(taken, cores)))

    give = functools.partial(give_back, where=where, labels=labels_list, shape=deltas.shape)
    starts = [first for first, _ in shares_of(width)]
    returned, rank = give(starts[0], values=values[0], ranked=(tail, *kept[0], labels_row))
    for chain in range(1, len(SHARES)):
        returned, = give(starts[chain], values=values[chain], returned=returned)
    return returned, rank.reshape(clients)


def solution(mesh):
    devices = mesh.shape["dp"] * mesh.shape["group"]
    placed = (P(AXES, None, None), P(AXES, None))

    def body(deltas, labels):
        return on_device(devices, deltas, labels)

    return jax.shard_map(
        body,
        mesh=mesh,
        in_specs=placed,
        out_specs=(P(AXES, None, None), P(AXES)),
        check_vma=False,
    )
```

```python
import functools

import jax
import jax.numpy as jnp
from jax import lax
from jax.experimental import pallas as pl
from jax.experimental.pallas import tpu as pltpu
from jax.sharding import PartitionSpec as P


CLUSTERS = 8
LANES = 128
AXES = ("dp", "group")
CHAINS = 2
COVER = 1 << 26

VMEM = pl.BlockSpec(memory_space=pltpu.VMEM)
SMEM = pl.BlockSpec(memory_space=pltpu.SMEM)
ANY = pl.BlockSpec(memory_space=pl.ANY)
HBM = pl.BlockSpec(memory_space=pltpu.HBM)


def role_of(index):
    for shift in (16, 8, 4, 2, 1):
        index = index ^ (index >> shift)
    return index & 1


def near(value):
    return pltpu.with_memory_space_constraint(value, pltpu.VMEM)


def far_off(value):
    return pltpu.with_memory_space_constraint(value, pltpu.HBM)


def count_rows(devices):
    return CLUSTERS * pl.cdiv(devices, LANES)


def bit_at(me, role, step):
    return (me >> (1 + (role ^ step))) & 1


def quarter_of(index):
    return (index >> 1) & 3


def local_sums_kernel(devices, chain, where, deltas, labels_row, other, mine, held, labels_here, sems):
    clients, blocks, _ = deltas.shape
    me = where[0]
    role = role_of(me)
    columns = held.shape[3]
    piece = columns // 2
    arrive = pltpu.make_async_copy(labels_row, labels_here, sems.at[8])
    arrive.start()
    copies = []
    for part in range(4):
        half = (1 - role) if part < 2 else role
        for second in range(2):
            owner = (part % 2) << (1 + half) | second << (2 - half)
            start = pl.multiple_of(((quarter_of(owner) * CHAINS + chain) * 2 + half) * piece, LANES)
            copies.append(pltpu.make_async_copy(
                deltas.at[:, :, pl.ds(start, piece)], held.at[part, :, :, second * piece:(second + 1) * piece],
                sems.at[part * 2 + second]))
            copies[-1].start()

    rows, depth = CLUSTERS * blocks, clients * blocks
    spread = (lax.broadcasted_iota(jnp.int32, (clients, depth), 1) // blocks
              == lax.broadcasted_iota(jnp.int32, (clients, depth), 0)).astype(jnp.bfloat16)
    row = lax.broadcasted_iota(jnp.int32, (rows, depth), 0)
    column = lax.broadcasted_iota(jnp.int32, (rows, depth), 1)
    same_row = column % blocks == row % blocks
    arrive.wait()
    labels = labels_here[...]
    wide = jnp.dot(jnp.broadcast_to(labels, (16, clients)).astype(jnp.bfloat16), spread,
                   preferred_element_type=jnp.float32)[0:1].astype(jnp.int32)
    pick = ((wide == row // blocks) & same_row).astype(jnp.bfloat16)

    hits = (labels == lax.broadcasted_iota(jnp.int32, (CLUSTERS, clients), 0)).astype(jnp.float32)
    counts = jnp.sum(hits, axis=1, keepdims=True)
    lane = lax.broadcasted_iota(jnp.int32, (CLUSTERS, LANES), 1)
    tail = count_rows(devices)
    for tile in range(tail // CLUSTERS):
        table = jnp.where(lane + tile * LANES == me, counts, 0.0)
        at = other.shape[0] - tail + tile * CLUSTERS
        other[at:at + CLUSTERS, :] = table
        mine[at:at + CLUSTERS, :] = table

    for part in range(4):
        copies[2 * part].wait()
        copies[2 * part + 1].wait()
        sums = jnp.dot(pick, held[part].reshape(depth, columns), preferred_element_type=jnp.float32)
        target = other if part < 2 else mine
        for block in range(columns // LANES):
            to = (part % 2 * columns // LANES + block) * rows
            target[to:to + rows, :] = sums[:, block * LANES:(block + 1) * LANES]


def local_sums(devices, chain, where, deltas, labels_row):
    clients, blocks, width = deltas.shape
    columns = width // (8 * CHAINS)
    height = 4 * columns // LANES * CLUSTERS * blocks + count_rows(devices)
    out = pltpu.VMEM((height, LANES), jnp.float32)
    return pl.pallas_call(
        functools.partial(local_sums_kernel, devices, chain),
        out_shape=(out, out),
        in_specs=[SMEM, HBM, HBM],
        out_specs=(VMEM, VMEM),
        scratch_shapes=[
            pltpu.VMEM((4, clients, blocks, 2 * columns), jnp.bfloat16), pltpu.VMEM((1, clients), jnp.int32),
            pltpu.SemaphoreType.DMA((9,))],
        compiler_params=pltpu.CompilerParams(vmem_limit_bytes=16 << 20),
        name="local_sums",
    )(where, far_off(deltas), far_off(labels_row))


def split_kernel(tail, step, where, kept, arrived, send, keep):
    half = (kept.shape[0] - tail) // 2
    bit = bit_at(where[0], role_of(where[0]), step)
    for target, which in ((send, 1 - bit), (keep, bit)):
        rows = pl.ds(pl.multiple_of(which * half, CLUSTERS), half)
        target[0:half, :] = kept[rows, :] + arrived[rows, :]
        target[half:half + tail, :] = kept[2 * half:2 * half + tail, :] + arrived[2 * half:2 * half + tail, :]


def split(tail, step, where, kept, arrived):
    half = (kept.shape[0] - tail) // 2
    out = pltpu.VMEM((half + tail, LANES), jnp.float32)
    return pl.pallas_call(
        functools.partial(split_kernel, tail, step),
        out_shape=(out, out),
        in_specs=[SMEM, VMEM, VMEM],
        out_specs=(VMEM, VMEM),
        compiler_params=pltpu.CompilerParams(vmem_limit_bytes=8 << 20),
        name="split",
    )(where, near(kept), near(arrived))


def table_of(tail, kept, arrived):
    ends = [kept.shape[0] - tail + at for at in range(0, tail, CLUSTERS)]
    return [kept[at:at + CLUSTERS, :] + arrived[at:at + CLUSTERS, :] for at in ends]


def finish_kernel(tail, blocks, kept, arrived, models):
    rows = CLUSTERS * blocks
    height = kept.shape[0] - tail
    totals = jnp.zeros((CLUSTERS, 1), jnp.float32)
    for counts in table_of(tail, kept, arrived):
        totals = totals + jnp.sum(counts, axis=1, keepdims=True)
    for cluster in range(CLUSTERS):
        total = jnp.broadcast_to(totals[cluster:cluster + 1, :], (blocks, LANES))
        for block in range(height // rows):
            at = block * rows + cluster * blocks
            sums = kept[at:at + blocks, :] + arrived[at:at + blocks, :]
            models[cluster * blocks:(cluster + 1) * blocks, block * LANES:(block + 1) * LANES] = (
                sums / total).astype(jnp.bfloat16)


def finish(tail, blocks, kept, arrived):
    rows = CLUSTERS * blocks
    columns = (kept.shape[0] - tail) // rows * LANES
    return pl.pallas_call(
        functools.partial(finish_kernel, tail, blocks),
        out_shape=pltpu.VMEM((rows, columns), jnp.bfloat16),
        in_specs=[VMEM, VMEM],
        out_specs=VMEM,
        compiler_params=pltpu.CompilerParams(vmem_limit_bytes=8 << 20),
        name="finish",
    )(near(kept), near(arrived))


def ranks_of(me, table, labels):
    clients = labels.shape[1]
    lane = lax.broadcasted_iota(jnp.int32, (CLUSTERS, LANES), 1)
    before = jnp.zeros((CLUSTERS, 1), jnp.float32)
    for tile, counts in enumerate(table):
        before = before + jnp.sum(jnp.where(lane + tile * LANES < me, counts, 0.0), axis=1, keepdims=True)
    hits = labels == lax.broadcasted_iota(jnp.int32, (CLUSTERS, clients), 0)
    earlier = (lax.broadcasted_iota(jnp.int32, (clients, clients), 0)
               < lax.broadcasted_iota(jnp.int32, (clients, clients), 1))
    local = jnp.dot(hits.astype(jnp.float32).astype(jnp.bfloat16), earlier.astype(jnp.float32).astype(jnp.bfloat16),
                    preferred_element_type=jnp.float32)
    return jnp.sum(jnp.where(hits, before + local, 0.0), axis=0, keepdims=True).astype(jnp.int32)


def own_places(me):
    return [(quarter_of(me), [
        (chain, other, chain, role_of(me) ^ other) for chain in range(CHAINS) for other in range(2)])]


def rest_places(me):
    role = role_of(me)
    kinds = [
        (me ^ 6, [(0, 0, role), (1, 0, 1 - role)]),
        (me ^ (2 << role), [(0, 1, role), (0, 2, 1 - role)]),
        (me ^ (4 >> role), [(1, 1, 1 - role), (1, 2, role)]),
    ]
    return [(quarter_of(chip), [
        (2 * chain + array, slot, chain, half) for chain in range(CHAINS) for array, slot, half in pieces])
        for chip, pieces in kinds]


def give_back_kernel(places, arrays, tail, where, labels, *rest):
    me = where[0]
    models, rest = rest[:arrays], rest[arrays:]
    if tail:
        kept, arrived, labels_row, returned, rank, laid, sem, rank_here, rank_sem = rest
    else:
        _, returned, laid, sem = rest
    columns = models[0].shape[2]
    clients, blocks, _ = returned.shape
    ends, offset = [], 0
    for at, (quarter, pieces) in enumerate(places(me)):
        size = len(pieces) * columns
        first = pieces[0][2]
        for array, slot, chain, half in pieces:
            to = offset + ((chain - first) * 2 + half) * columns
            to = pl.ds(pl.multiple_of(to, LANES), columns)
            for cluster in range(CLUSTERS):
                laid[cluster, :, to] = models[array][slot, cluster * blocks:(cluster + 1) * blocks, :]
        across = pl.ds(pl.multiple_of((quarter * CHAINS + first) * 2 * columns, LANES), size)
        for client in range(clients):
            pltpu.make_async_copy(
                laid.at[labels[client], :, offset:offset + size], returned.at[client, :, across], sem.at[at]).start()
        whole = returned.at[:, :, across]
        ends.append(pltpu.make_async_copy(whole, whole, sem.at[at]))
        offset += size
    if tail:
        rank_here[...] = ranks_of(me, table_of(tail, kept, arrived), labels_row[...])
        ends.append(pltpu.make_async_copy(rank_here, rank, rank_sem))
        ends[-1].start()
    for end in ends:
        end.wait()


def give_back(places, where, labels, models, shape, returned=None, ranked=None):
    columns = models[0].shape[2]
    slots = sum(array.shape[0] for array in models)
    scratch = [pltpu.VMEM((CLUSTERS, shape[1], slots * columns), jnp.bfloat16), pltpu.SemaphoreType.DMA((3,))]
    out = [jax.ShapeDtypeStruct(shape, jnp.bfloat16)]
    if ranked is None:
        tail, more, more_specs, aliases = 0, (returned,), [ANY], {2 + len(models): 0}
    else:
        tail, kept, arrived, labels_row = ranked
        more, more_specs, aliases = (near(kept), near(arrived), near(labels_row)), [VMEM] * 3, {}
        out.append(jax.ShapeDtypeStruct(labels_row.shape, jnp.int32))
        scratch += [pltpu.VMEM(labels_row.shape, jnp.int32), pltpu.SemaphoreType.DMA]
    return pl.pallas_call(
        functools.partial(give_back_kernel, places, len(models), tail),
        out_shape=out,
        in_specs=[SMEM, SMEM] + [VMEM] * len(models) + more_specs,
        out_specs=[ANY] * len(out),
        scratch_shapes=scratch,
        input_output_aliases=aliases,
        compiler_params=pltpu.CompilerParams(vmem_limit_bytes=8 << 20),
        cost_estimate=pl.CostEstimate(flops=COVER, bytes_accessed=0, transcendentals=0),
        name="give_back",
    )(where, labels, *[near(array) for array in models], *more)


def on_device(devices, deltas, labels):
    clients, blocks, _ = deltas.shape
    where = lax.axis_index(AXES).astype(jnp.int32).reshape(1)
    labels_row = labels.reshape(1, clients)
    labels_list = labels.reshape(clients)
    tail = count_rows(devices)
    bits = devices.bit_length() - 1

    def send(value, flip):
        return lax.ppermute(value, AXES, [(i, i ^ flip(i)) for i in range(devices)])

    def cores(i):
        return 1

    def crossed(low, high, step):
        def flip(i):
            return 1 << (high - 1 - step if role_of(i) else low + step) | 1

        return flip

    kept = []
    for chain in range(CHAINS):
        other, mine = local_sums(devices, chain, where, deltas, labels_row)
        kept.append(split(tail, 0, where, mine, send(other, cores)))
    for chain, (out, keep) in enumerate(kept):
        kept[chain] = split(tail, 1, where, keep, send(out, crossed(1, 3, 0)))
    for chain, (out, keep) in enumerate(kept):
        kept[chain] = (keep, send(out, crossed(1, 3, 1)))
    for step in range(bits - 3):
        for chain, (keep, arrived) in enumerate(kept):
            total = keep + arrived
            kept[chain] = (total, send(total, crossed(3, bits, step)))
    pairs, rests = [], []
    for pair in kept:
        own = finish(tail, blocks, *pair)[None]
        diagonal = send(own, lambda i: 6)
        pairs.append(jnp.concatenate([own, send(own, cores)], axis=0))
        beside = send(pairs[-1], lambda i: 2 << role_of(i) | 1)
        taken = jnp.concatenate([diagonal, beside], axis=0)
        rests.append([taken, send(taken, cores)])

    give = functools.partial(give_back, where=where, labels=labels_list, shape=deltas.shape)
    returned, rank = give(own_places, models=pairs, ranked=(tail, *kept[0], labels_row))
    returned, = give(rest_places, models=rests[0] + rests[1], returned=returned)
    return returned, rank.reshape(clients)


def solution(mesh):
    devices = mesh.shape["dp"] * mesh.shape["group"]
    placed = (P(AXES, None, None), P(AXES, None))

    def body(deltas, labels):
        return on_device(devices, deltas, labels)

    return jax.shard_map(
        body,
        mesh=mesh,
        in_specs=placed,
        out_specs=(P(AXES, None, None), P(AXES)),
        check_vma=False,
    )
```

```python
import functools

import jax
import jax.numpy as jnp
from jax import lax
from jax.experimental import pallas as pl
from jax.experimental.pallas import tpu as pltpu
from jax.sharding import PartitionSpec as P


CLUSTERS = 8
LANES = 128
AXES = ("dp", "group")
CHAINS = 2
COVER = 1 << 26

VMEM = pl.BlockSpec(memory_space=pltpu.VMEM)
SMEM = pl.BlockSpec(memory_space=pltpu.SMEM)
ANY = pl.BlockSpec(memory_space=pl.ANY)
HBM = pl.BlockSpec(memory_space=pltpu.HBM)


def role_of(index):
    for shift in (16, 8, 4, 2, 1):
        index = index ^ (index >> shift)
    return index & 1


def near(value):
    return pltpu.with_memory_space_constraint(value, pltpu.VMEM)


def far_off(value):
    return pltpu.with_memory_space_constraint(value, pltpu.HBM)


def count_rows(devices):
    return CLUSTERS * pl.cdiv(devices, LANES)


def bit_at(me, role, step):
    return (me >> (1 + (role ^ step))) & 1


def quarter_of(index):
    return (index >> 1) & 3


def local_sums_kernel(devices, chain, where, deltas, labels_row, other, mine, held, labels_here, sems):
    clients, blocks, _ = deltas.shape
    me = where[0]
    role = role_of(me)
    columns = held.shape[3]
    piece = columns // 2
    arrive = pltpu.make_async_copy(labels_row, labels_here, sems.at[8])
    arrive.start()
    copies = []
    for part in range(4):
        half = (1 - role) if part < 2 else role
        for second in range(2):
            owner = (part % 2) << (1 + half) | second << (2 - half)
            start = pl.multiple_of(((quarter_of(owner) * CHAINS + chain) * 2 + half) * piece, LANES)
            copies.append(pltpu.make_async_copy(
                deltas.at[:, :, pl.ds(start, piece)], held.at[part, :, :, second * piece:(second + 1) * piece],
                sems.at[part * 2 + second]))
            copies[-1].start()

    rows, depth = CLUSTERS * blocks, clients * blocks
    spread = (lax.broadcasted_iota(jnp.int32, (clients, depth), 1) // blocks
              == lax.broadcasted_iota(jnp.int32, (clients, depth), 0)).astype(jnp.bfloat16)
    row = lax.broadcasted_iota(jnp.int32, (rows, depth), 0)
    column = lax.broadcasted_iota(jnp.int32, (rows, depth), 1)
    same_row = column % blocks == row % blocks
    arrive.wait()
    labels = labels_here[...]
    wide = jnp.dot(jnp.broadcast_to(labels, (16, clients)).astype(jnp.bfloat16), spread,
                   preferred_element_type=jnp.float32)[0:1].astype(jnp.int32)
    pick = ((wide == row // blocks) & same_row).astype(jnp.bfloat16)

    hits = (labels == lax.broadcasted_iota(jnp.int32, (CLUSTERS, clients), 0)).astype(jnp.float32)
    counts = jnp.sum(hits, axis=1, keepdims=True)
    lane = lax.broadcasted_iota(jnp.int32, (CLUSTERS, LANES), 1)
    tail = count_rows(devices)
    for tile in range(tail // CLUSTERS):
        table = jnp.where(lane + tile * LANES == me, counts, 0.0)
        at = other.shape[0] - tail + tile * CLUSTERS
        other[at:at + CLUSTERS, :] = table
        mine[at:at + CLUSTERS, :] = table

    for part in range(4):
        copies[2 * part].wait()
        copies[2 * part + 1].wait()
        sums = jnp.dot(pick, held[part].reshape(depth, columns), preferred_element_type=jnp.float32)
        target = other if part < 2 else mine
        for block in range(columns // LANES):
            to = (part % 2 * columns // LANES + block) * rows
            target[to:to + rows, :] = sums[:, block * LANES:(block + 1) * LANES]


def local_sums(devices, chain, where, deltas, labels_row):
    clients, blocks, width = deltas.shape
    columns = width // (8 * CHAINS)
    height = 4 * columns // LANES * CLUSTERS * blocks + count_rows(devices)
    out = pltpu.VMEM((height, LANES), jnp.float32)
    return pl.pallas_call(
        functools.partial(local_sums_kernel, devices, chain),
        out_shape=(out, out),
        in_specs=[SMEM, HBM, HBM],
        out_specs=(VMEM, VMEM),
        scratch_shapes=[
            pltpu.VMEM((4, clients, blocks, 2 * columns), jnp.bfloat16), pltpu.VMEM((1, clients), jnp.int32),
            pltpu.SemaphoreType.DMA((9,))],
        compiler_params=pltpu.CompilerParams(vmem_limit_bytes=16 << 20),
        name="local_sums",
    )(where, far_off(deltas), far_off(labels_row))


def split_kernel(tail, step, where, kept, arrived, send, keep):
    half = (kept.shape[0] - tail) // 2
    bit = bit_at(where[0], role_of(where[0]), step)
    for target, which in ((send, 1 - bit), (keep, bit)):
        rows = pl.ds(pl.multiple_of(which * half, CLUSTERS), half)
        target[0:half, :] = kept[rows, :] + arrived[rows, :]
        target[half:half + tail, :] = kept[2 * half:2 * half + tail, :] + arrived[2 * half:2 * half + tail, :]


def split(tail, step, where, kept, arrived):
    half = (kept.shape[0] - tail) // 2
    out = pltpu.VMEM((half + tail, LANES), jnp.float32)
    return pl.pallas_call(
        functools.partial(split_kernel, tail, step),
        out_shape=(out, out),
        in_specs=[SMEM, VMEM, VMEM],
        out_specs=(VMEM, VMEM),
        compiler_params=pltpu.CompilerParams(vmem_limit_bytes=8 << 20),
        name="split",
    )(where, near(kept), near(arrived))


def table_of(tail, kept, arrived):
    ends = [kept.shape[0] - tail + at for at in range(0, tail, CLUSTERS)]
    return [kept[at:at + CLUSTERS, :] + arrived[at:at + CLUSTERS, :] for at in ends]


def finish_kernel(tail, blocks, kept, arrived, models):
    rows = CLUSTERS * blocks
    height = kept.shape[0] - tail
    totals = jnp.zeros((CLUSTERS, 1), jnp.float32)
    for counts in table_of(tail, kept, arrived):
        totals = totals + jnp.sum(counts, axis=1, keepdims=True)
    for cluster in range(CLUSTERS):
        total = jnp.broadcast_to(totals[cluster:cluster + 1, :], (blocks, LANES))
        for block in range(height // rows):
            at = block * rows + cluster * blocks
            sums = kept[at:at + blocks, :] + arrived[at:at + blocks, :]
            models[cluster * blocks:(cluster + 1) * blocks, block * LANES:(block + 1) * LANES] = (
                sums / total).astype(jnp.bfloat16)


def finish(tail, blocks, kept, arrived):
    rows = CLUSTERS * blocks
    columns = (kept.shape[0] - tail) // rows * LANES
    return pl.pallas_call(
        functools.partial(finish_kernel, tail, blocks),
        out_shape=pltpu.VMEM((rows, columns), jnp.bfloat16),
        in_specs=[VMEM, VMEM],
        out_specs=VMEM,
        compiler_params=pltpu.CompilerParams(vmem_limit_bytes=8 << 20),
        name="finish",
    )(near(kept), near(arrived))


def join_kernel(*refs):
    at = 0
    for part in refs[:-1]:
        refs[-1][at:at + part.shape[0]] = part[...]
        at += part.shape[0]


def join(*parts):
    slots = sum(part.shape[0] for part in parts)
    return pl.pallas_call(
        join_kernel,
        out_shape=pltpu.VMEM((slots,) + parts[0].shape[1:], parts[0].dtype),
        in_specs=[VMEM] * len(parts),
        out_specs=VMEM,
        compiler_params=pltpu.CompilerParams(vmem_limit_bytes=8 << 20),
        name="join",
    )(*[near(part) for part in parts])


def ranks_of(me, table, labels):
    clients = labels.shape[1]
    lane = lax.broadcasted_iota(jnp.int32, (CLUSTERS, LANES), 1)
    before = jnp.zeros((CLUSTERS, 1), jnp.float32)
    for tile, counts in enumerate(table):
        before = before + jnp.sum(jnp.where(lane + tile * LANES < me, counts, 0.0), axis=1, keepdims=True)
    hits = labels == lax.broadcasted_iota(jnp.int32, (CLUSTERS, clients), 0)
    earlier = (lax.broadcasted_iota(jnp.int32, (clients, clients), 0)
               < lax.broadcasted_iota(jnp.int32, (clients, clients), 1))
    local = jnp.dot(hits.astype(jnp.float32).astype(jnp.bfloat16), earlier.astype(jnp.float32).astype(jnp.bfloat16),
                    preferred_element_type=jnp.float32)
    return jnp.sum(jnp.where(hits, before + local, 0.0), axis=0, keepdims=True).astype(jnp.int32)


def own_places(me):
    return [(quarter_of(me), [
        (chain, other, chain, role_of(me) ^ other) for chain in range(CHAINS) for other in range(2)])]


def rest_places(me):
    role = role_of(me)
    kinds = [
        (me ^ 6, [(0, 0, role), (1, 0, 1 - role)]),
        (me ^ (2 << role), [(0, 1, role), (0, 2, 1 - role)]),
        (me ^ (4 >> role), [(1, 1, 1 - role), (1, 2, role)]),
    ]
    return [(quarter_of(chip), [
        (2 * chain + array, slot, chain, half) for chain in range(CHAINS) for array, slot, half in pieces])
        for chip, pieces in kinds]


def give_back_kernel(places, arrays, tail, where, labels, *rest):
    me = where[0]
    models, rest = rest[:arrays], rest[arrays:]
    if tail:
        kept, arrived, labels_row, returned, rank, laid, sem, rank_here, rank_sem = rest
    else:
        _, returned, laid, sem = rest
    columns = models[0].shape[2]
    clients, blocks, _ = returned.shape
    ends, offset = [], 0
    for at, (quarter, pieces) in enumerate(places(me)):
        size = len(pieces) * columns
        first = pieces[0][2]
        for array, slot, chain, half in pieces:
            to = offset + ((chain - first) * 2 + half) * columns
            to = pl.ds(pl.multiple_of(to, LANES), columns)
            for cluster in range(CLUSTERS):
                laid[cluster, :, to] = models[array][slot, cluster * blocks:(cluster + 1) * blocks, :]
        across = pl.ds(pl.multiple_of((quarter * CHAINS + first) * 2 * columns, LANES), size)
        for client in range(clients):
            pltpu.make_async_copy(
                laid.at[labels[client], :, offset:offset + size], returned.at[client, :, across], sem.at[at]).start()
        whole = returned.at[:, :, across]
        ends.append(pltpu.make_async_copy(whole, whole, sem.at[at]))
        offset += size
    if tail:
        rank_here[...] = ranks_of(me, table_of(tail, kept, arrived), labels_row[...])
        ends.append(pltpu.make_async_copy(rank_here, rank, rank_sem))
        ends[-1].start()
    for end in ends:
        end.wait()


def give_back(places, where, labels, models, shape, returned=None, ranked=None):
    columns = models[0].shape[2]
    slots = sum(array.shape[0] for array in models)
    scratch = [pltpu.VMEM((CLUSTERS, shape[1], slots * columns), jnp.bfloat16), pltpu.SemaphoreType.DMA((3,))]
    out = [jax.ShapeDtypeStruct(shape, jnp.bfloat16)]
    if ranked is None:
        tail, more, more_specs, aliases = 0, (returned,), [ANY], {2 + len(models): 0}
    else:
        tail, kept, arrived, labels_row = ranked
        more, more_specs, aliases = (near(kept), near(arrived), near(labels_row)), [VMEM] * 3, {}
        out.append(jax.ShapeDtypeStruct(labels_row.shape, jnp.int32))
        scratch += [pltpu.VMEM(labels_row.shape, jnp.int32), pltpu.SemaphoreType.DMA]
    return pl.pallas_call(
        functools.partial(give_back_kernel, places, len(models), tail),
        out_shape=out,
        in_specs=[SMEM, SMEM] + [VMEM] * len(models) + more_specs,
        out_specs=[ANY] * len(out),
        scratch_shapes=scratch,
        input_output_aliases=aliases,
        compiler_params=pltpu.CompilerParams(vmem_limit_bytes=8 << 20),
        cost_estimate=pl.CostEstimate(flops=COVER, bytes_accessed=0, transcendentals=0),
        name="give_back",
    )(where, labels, *[near(array) for array in models], *more)


def on_device(devices, deltas, labels):
    clients, blocks, _ = deltas.shape
    where = lax.axis_index(AXES).astype(jnp.int32).reshape(1)
    labels_row = labels.reshape(1, clients)
    labels_list = labels.reshape(clients)
    tail = count_rows(devices)
    bits = devices.bit_length() - 1

    def send(value, flip):
        return lax.ppermute(value, AXES, [(i, i ^ flip(i)) for i in range(devices)])

    def cores(i):
        return 1

    def crossed(low, high, step):
        def flip(i):
            return 1 << (high - 1 - step if role_of(i) else low + step) | 1

        return flip

    kept = []
    for chain in range(CHAINS):
        other, mine = local_sums(devices, chain, where, deltas, labels_row)
        kept.append(split(tail, 0, where, mine, send(other, cores)))
    for chain, (out, keep) in enumerate(kept):
        kept[chain] = split(tail, 1, where, keep, send(out, crossed(1, 3, 0)))
    for chain, (out, keep) in enumerate(kept):
        kept[chain] = (keep, send(out, crossed(1, 3, 1)))
    for step in range(bits - 3):
        for chain, (keep, arrived) in enumerate(kept):
            total = keep + arrived
            kept[chain] = (total, send(total, crossed(3, bits, step)))
    pairs, rests = [], []
    for pair in kept:
        own = finish(tail, blocks, *pair)[None]
        diagonal = send(own, lambda i: 6)
        pairs.append(join(own, send(own, cores)))
        beside = send(pairs[-1], lambda i: 2 << role_of(i) | 1)
        taken = join(diagonal, beside)
        rests.append([taken, send(taken, cores)])

    give = functools.partial(give_back, where=where, labels=labels_list, shape=deltas.shape)
    returned, rank = give(own_places, models=pairs, ranked=(tail, *kept[0], labels_row))
    returned, = give(rest_places, models=rests[0] + rests[1], returned=returned)
    return returned, rank.reshape(clients)


def solution(mesh):
    devices = mesh.shape["dp"] * mesh.shape["group"]
    placed = (P(AXES, None, None), P(AXES, None))

    def body(deltas, labels):
        return on_device(devices, deltas, labels)

    return jax.shard_map(
        body,
        mesh=mesh,
        in_specs=placed,
        out_specs=(P(AXES, None, None), P(AXES)),
        check_vma=False,
    )
```

```python
import functools

import jax
import jax.numpy as jnp
from jax import lax
from jax.experimental import pallas as pl
from jax.experimental.pallas import tpu as pltpu
from jax.sharding import PartitionSpec as P


CLUSTERS = 8
LANES = 128
AXES = ("dp", "group")
CHAINS = 2
COVER = 1 << 26

VMEM = pl.BlockSpec(memory_space=pltpu.VMEM)
SMEM = pl.BlockSpec(memory_space=pltpu.SMEM)
ANY = pl.BlockSpec(memory_space=pl.ANY)
HBM = pl.BlockSpec(memory_space=pltpu.HBM)


def role_of(index):
    for shift in (16, 8, 4, 2, 1):
        index = index ^ (index >> shift)
    return index & 1


def near(value):
    return pltpu.with_memory_space_constraint(value, pltpu.VMEM)


def far_off(value):
    return pltpu.with_memory_space_constraint(value, pltpu.HBM)


def count_rows(devices):
    return CLUSTERS * pl.cdiv(devices, LANES)


def bit_at(me, role, step):
    return (me >> (1 + (role ^ step))) & 1


def quarter_of(index):
    return (index >> 1) & 3


def local_sums_kernel(devices, chain, where, deltas, labels_row, other, mine, held, labels_here, sems):
    clients, blocks, _ = deltas.shape
    me = where[0]
    role = role_of(me)
    columns = held.shape[3]
    piece = columns // 2
    arrive = pltpu.make_async_copy(labels_row, labels_here, sems.at[8])
    arrive.start()
    copies = []
    for part in range(4):
        half = (1 - role) if part < 2 else role
        for second in range(2):
            owner = (part % 2) << (1 + half) | second << (2 - half)
            start = pl.multiple_of(((quarter_of(owner) * CHAINS + chain) * 2 + half) * piece, LANES)
            copies.append(pltpu.make_async_copy(
                deltas.at[:, :, pl.ds(start, piece)], held.at[part, :, :, second * piece:(second + 1) * piece],
                sems.at[part * 2 + second]))
            copies[-1].start()

    rows, depth = CLUSTERS * blocks, clients * blocks
    spread = (lax.broadcasted_iota(jnp.int32, (clients, depth), 1) // blocks
              == lax.broadcasted_iota(jnp.int32, (clients, depth), 0)).astype(jnp.bfloat16)
    row = lax.broadcasted_iota(jnp.int32, (rows, depth), 0)
    column = lax.broadcasted_iota(jnp.int32, (rows, depth), 1)
    same_row = column % blocks == row % blocks
    arrive.wait()
    labels = labels_here[...]
    wide = jnp.dot(jnp.broadcast_to(labels, (16, clients)).astype(jnp.bfloat16), spread,
                   preferred_element_type=jnp.float32)[0:1].astype(jnp.int32)
    pick = ((wide == row // blocks) & same_row).astype(jnp.bfloat16)

    hits = (labels == lax.broadcasted_iota(jnp.int32, (CLUSTERS, clients), 0)).astype(jnp.float32)
    counts = jnp.sum(hits, axis=1, keepdims=True)
    lane = lax.broadcasted_iota(jnp.int32, (CLUSTERS, LANES), 1)
    tail = count_rows(devices)
    for tile in range(tail // CLUSTERS):
        table = jnp.where(lane + tile * LANES == me, counts, 0.0)
        at = other.shape[0] - tail + tile * CLUSTERS
        other[at:at + CLUSTERS, :] = table
        mine[at:at + CLUSTERS, :] = table

    for part in range(4):
        copies[2 * part].wait()
        copies[2 * part + 1].wait()
        sums = jnp.dot(pick, held[part].reshape(depth, columns), preferred_element_type=jnp.float32)
        target = other if part < 2 else mine
        for block in range(columns // LANES):
            to = (part % 2 * columns // LANES + block) * rows
            target[to:to + rows, :] = sums[:, block * LANES:(block + 1) * LANES]


def local_sums(devices, chain, where, deltas, labels_row):
    clients, blocks, width = deltas.shape
    columns = width // (8 * CHAINS)
    height = 4 * columns // LANES * CLUSTERS * blocks + count_rows(devices)
    out = pltpu.VMEM((height, LANES), jnp.float32)
    return pl.pallas_call(
        functools.partial(local_sums_kernel, devices, chain),
        out_shape=(out, out),
        in_specs=[SMEM, HBM, HBM],
        out_specs=(VMEM, VMEM),
        scratch_shapes=[
            pltpu.VMEM((4, clients, blocks, 2 * columns), jnp.bfloat16), pltpu.VMEM((1, clients), jnp.int32),
            pltpu.SemaphoreType.DMA((9,))],
        compiler_params=pltpu.CompilerParams(vmem_limit_bytes=16 << 20),
        name="local_sums",
    )(where, far_off(deltas), far_off(labels_row))


def split_kernel(tail, step, where, kept, arrived, send, keep):
    half = (kept.shape[0] - tail) // 2
    bit = bit_at(where[0], role_of(where[0]), step)
    for target, which in ((send, 1 - bit), (keep, bit)):
        rows = pl.ds(pl.multiple_of(which * half, CLUSTERS), half)
        target[0:half, :] = kept[rows, :] + arrived[rows, :]
        target[half:half + tail, :] = kept[2 * half:2 * half + tail, :] + arrived[2 * half:2 * half + tail, :]


def split(tail, step, where, kept, arrived):
    half = (kept.shape[0] - tail) // 2
    out = pltpu.VMEM((half + tail, LANES), jnp.float32)
    return pl.pallas_call(
        functools.partial(split_kernel, tail, step),
        out_shape=(out, out),
        in_specs=[SMEM, VMEM, VMEM],
        out_specs=(VMEM, VMEM),
        compiler_params=pltpu.CompilerParams(vmem_limit_bytes=8 << 20),
        name="split",
    )(where, near(kept), near(arrived))


def table_of(tail, kept, arrived):
    ends = [kept.shape[0] - tail + at for at in range(0, tail, CLUSTERS)]
    return [kept[at:at + CLUSTERS, :] + arrived[at:at + CLUSTERS, :] for at in ends]


def finish_kernel(tail, blocks, kept, arrived, models):
    rows = CLUSTERS * blocks
    height = kept.shape[0] - tail
    totals = jnp.zeros((CLUSTERS, 1), jnp.float32)
    for counts in table_of(tail, kept, arrived):
        totals = totals + jnp.sum(counts, axis=1, keepdims=True)
    for cluster in range(CLUSTERS):
        total = jnp.broadcast_to(totals[cluster:cluster + 1, :], (blocks, LANES))
        for block in range(height // rows):
            at = block * rows + cluster * blocks
            sums = kept[at:at + blocks, :] + arrived[at:at + blocks, :]
            models[cluster * blocks:(cluster + 1) * blocks, block * LANES:(block + 1) * LANES] = (
                sums / total).astype(jnp.bfloat16)


def finish(tail, blocks, kept, arrived):
    rows = CLUSTERS * blocks
    columns = (kept.shape[0] - tail) // rows * LANES
    return pl.pallas_call(
        functools.partial(finish_kernel, tail, blocks),
        out_shape=pltpu.VMEM((rows, columns), jnp.bfloat16),
        in_specs=[VMEM, VMEM],
        out_specs=VMEM,
        compiler_params=pltpu.CompilerParams(vmem_limit_bytes=8 << 20),
        name="finish",
    )(near(kept), near(arrived))


def join_kernel(*refs):
    at = 0
    for part in refs[:-1]:
        refs[-1][at:at + part.shape[0]] = part[...]
        at += part.shape[0]


def join(*parts):
    slots = sum(part.shape[0] for part in parts)
    return pl.pallas_call(
        join_kernel,
        out_shape=pltpu.VMEM((slots,) + parts[0].shape[1:], parts[0].dtype),
        in_specs=[VMEM] * len(parts),
        out_specs=VMEM,
        compiler_params=pltpu.CompilerParams(vmem_limit_bytes=8 << 20),
        name="join",
    )(*[near(part) for part in parts])


def ranks_of(me, table, labels):
    clients = labels.shape[1]
    lane = lax.broadcasted_iota(jnp.int32, (CLUSTERS, LANES), 1)
    before = jnp.zeros((CLUSTERS, 1), jnp.float32)
    for tile, counts in enumerate(table):
        before = before + jnp.sum(jnp.where(lane + tile * LANES < me, counts, 0.0), axis=1, keepdims=True)
    hits = labels == lax.broadcasted_iota(jnp.int32, (CLUSTERS, clients), 0)
    earlier = (lax.broadcasted_iota(jnp.int32, (clients, clients), 0)
               < lax.broadcasted_iota(jnp.int32, (clients, clients), 1))
    local = jnp.dot(hits.astype(jnp.float32).astype(jnp.bfloat16), earlier.astype(jnp.float32).astype(jnp.bfloat16),
                    preferred_element_type=jnp.float32)
    return jnp.sum(jnp.where(hits, before + local, 0.0), axis=0, keepdims=True).astype(jnp.int32)


def early_places(me):
    role = role_of(me)
    return [
        (quarter_of(me), [(chain, other, chain, role ^ other) for chain in range(CHAINS) for other in range(2)]),
        (quarter_of(me ^ (2 << role)), [(CHAINS, 1, 0, role), (CHAINS, 2, 0, 1 - role)]),
        (quarter_of(me ^ 6), [(CHAINS, 0, 0, role)]),
    ]


def late_places(me):
    role = role_of(me)
    return [
        (quarter_of(me ^ (4 >> role)), [
            (2 * chain, slot, chain, role ^ other) for chain in range(CHAINS) for slot, other in ((1, 1), (2, 0))]),
        (quarter_of(me ^ (2 << role)), [(1, 1, 1, role), (1, 2, 1, 1 - role)]),
        (quarter_of(me ^ 6), [(1, 0, 1, role), (2, 0, 1, 1 - role)]),
        (quarter_of(me ^ 6), [(0, 0, 0, 1 - role)]),
    ]


def give_back_kernel(places, arrays, tail, where, labels, *rest):
    me = where[0]
    models, rest = rest[:arrays], rest[arrays:]
    if tail:
        kept, arrived, labels_row, returned, rank, laid, sem, rank_here, rank_sem = rest
    else:
        _, returned, laid, sem = rest
    columns = models[0].shape[2]
    clients, blocks, _ = returned.shape
    ends, offset = [], 0
    for at, (quarter, pieces) in enumerate(places(me)):
        size = len(pieces) * columns
        first = pieces[0][2] * 2 + (pieces[0][3] if len(pieces) == 1 else 0)
        for array, slot, chain, half in pieces:
            to = offset + (chain * 2 + half - first) * columns
            to = pl.ds(pl.multiple_of(to, LANES), columns)
            for cluster in range(CLUSTERS):
                laid[cluster, :, to] = models[array][slot, cluster * blocks:(cluster + 1) * blocks, :]
        across = pl.ds(pl.multiple_of((quarter * CHAINS * 2 + first) * columns, LANES), size)
        for client in range(clients):
            pltpu.make_async_copy(
                laid.at[labels[client], :, offset:offset + size], returned.at[client, :, across], sem.at[at]).start()
        whole = returned.at[:, :, across]
        ends.append(pltpu.make_async_copy(whole, whole, sem.at[at]))
        offset += size
    if tail:
        rank_here[...] = ranks_of(me, table_of(tail, kept, arrived), labels_row[...])
        ends.append(pltpu.make_async_copy(rank_here, rank, rank_sem))
        ends[-1].start()
    for end in ends:
        end.wait()


def give_back(places, where, labels, models, shape, returned=None, ranked=None):
    columns = models[0].shape[2]
    slots = sum(array.shape[0] for array in models)
    scratch = [pltpu.VMEM((CLUSTERS, shape[1], slots * columns), jnp.bfloat16), pltpu.SemaphoreType.DMA((4,))]
    out = [jax.ShapeDtypeStruct(shape, jnp.bfloat16)]
    if ranked is None:
        tail, more, more_specs, aliases = 0, (returned,), [ANY], {2 + len(models): 0}
    else:
        tail, kept, arrived, labels_row = ranked
        more, more_specs, aliases = (near(kept), near(arrived), near(labels_row)), [VMEM] * 3, {}
        out.append(jax.ShapeDtypeStruct(labels_row.shape, jnp.int32))
        scratch += [pltpu.VMEM(labels_row.shape, jnp.int32), pltpu.SemaphoreType.DMA]
    return pl.pallas_call(
        functools.partial(give_back_kernel, places, len(models), tail),
        out_shape=out,
        in_specs=[SMEM, SMEM] + [VMEM] * len(models) + more_specs,
        out_specs=[ANY] * len(out),
        scratch_shapes=scratch,
        input_output_aliases=aliases,
        compiler_params=pltpu.CompilerParams(vmem_limit_bytes=8 << 20),
        cost_estimate=pl.CostEstimate(flops=COVER, bytes_accessed=0, transcendentals=0),
        name="give_back",
    )(where, labels, *[near(array) for array in models], *more)


def on_device(devices, deltas, labels):
    clients, blocks, _ = deltas.shape
    where = lax.axis_index(AXES).astype(jnp.int32).reshape(1)
    labels_row = labels.reshape(1, clients)
    labels_list = labels.reshape(clients)
    tail = count_rows(devices)
    bits = devices.bit_length() - 1

    def send(value, flip):
        return lax.ppermute(value, AXES, [(i, i ^ flip(i)) for i in range(devices)])

    def cores(i):
        return 1

    def crossed(low, high, step):
        def flip(i):
            return 1 << (high - 1 - step if role_of(i) else low + step) | 1

        return flip

    kept = []
    for chain in range(CHAINS):
        other, mine = local_sums(devices, chain, where, deltas, labels_row)
        kept.append(split(tail, 0, where, mine, send(other, cores)))
    for chain, (out, keep) in enumerate(kept):
        kept[chain] = split(tail, 1, where, keep, send(out, crossed(1, 3, 0)))
    for chain, (out, keep) in enumerate(kept):
        kept[chain] = (keep, send(out, crossed(1, 3, 1)))
    for step in range(bits - 3):
        for chain, (keep, arrived) in enumerate(kept):
            total = keep + arrived
            kept[chain] = (total, send(total, crossed(3, bits, step)))
    pairs, rests = [], []
    for pair in kept:
        own = finish(tail, blocks, *pair)[None]
        diagonal = send(own, lambda i: 6)
        pairs.append(join(own, send(own, cores)))
        beside = send(pairs[-1], lambda i: 2 << role_of(i) | 1)
        taken = join(diagonal, beside)
        rests.append([taken, send(taken, cores)])

    give = functools.partial(give_back, where=where, labels=labels_list, shape=deltas.shape)
    returned, rank = give(early_places, models=pairs + rests[0][:1], ranked=(tail, *kept[0], labels_row))
    returned, = give(late_places, models=rests[0][1:] + rests[1], returned=returned)
    return returned, rank.reshape(clients)


def solution(mesh):
    devices = mesh.shape["dp"] * mesh.shape["group"]
    placed = (P(AXES, None, None), P(AXES, None))

    def body(deltas, labels):
        return on_device(devices, deltas, labels)

    return jax.shard_map(
        body,
        mesh=mesh,
        in_specs=placed,
        out_specs=(P(AXES, None, None), P(AXES)),
        check_vma=False,
    )
```

```python
import functools

import jax
import jax.numpy as jnp
from jax import lax
from jax.experimental import pallas as pl
from jax.experimental.pallas import tpu as pltpu
from jax.sharding import PartitionSpec as P


CLUSTERS = 8
LANES = 128
AXES = ("dp", "group")
CHAINS = 2
COVER = 1 << 26

VMEM = pl.BlockSpec(memory_space=pltpu.VMEM)
SMEM = pl.BlockSpec(memory_space=pltpu.SMEM)
ANY = pl.BlockSpec(memory_space=pl.ANY)
HBM = pl.BlockSpec(memory_space=pltpu.HBM)


def role_of(index):
    for shift in (16, 8, 4, 2, 1):
        index = index ^ (index >> shift)
    return index & 1


def near(value):
    return pltpu.with_memory_space_constraint(value, pltpu.VMEM)


def far_off(value):
    return pltpu.with_memory_space_constraint(value, pltpu.HBM)


def count_rows(devices):
    return CLUSTERS * pl.cdiv(devices, LANES)


def bit_at(me, role, step):
    return (me >> (1 + (role ^ step))) & 1


def quarter_of(index):
    return (index >> 1) & 3


def local_sums_kernel(tail, chain, where, deltas, labels_row, other, mine, held, labels_here, sems):
    clients, blocks, _ = deltas.shape
    me = where[0]
    role = role_of(me)
    columns = held.shape[3]
    piece = columns // 2
    arrive = pltpu.make_async_copy(labels_row, labels_here, sems.at[8])
    arrive.start()
    copies = []
    for part in range(4):
        half = (1 - role) if part < 2 else role
        for second in range(2):
            owner = (part % 2) << (1 + half) | second << (2 - half)
            start = pl.multiple_of(((quarter_of(owner) * CHAINS + chain) * 2 + half) * piece, LANES)
            copies.append(pltpu.make_async_copy(
                deltas.at[:, :, pl.ds(start, piece)], held.at[part, :, :, second * piece:(second + 1) * piece],
                sems.at[part * 2 + second]))
            copies[-1].start()

    rows, depth = CLUSTERS * blocks, clients * blocks
    spread = (lax.broadcasted_iota(jnp.int32, (clients, depth), 1) // blocks
              == lax.broadcasted_iota(jnp.int32, (clients, depth), 0)).astype(jnp.bfloat16)
    row = lax.broadcasted_iota(jnp.int32, (rows, depth), 0)
    column = lax.broadcasted_iota(jnp.int32, (rows, depth), 1)
    same_row = column % blocks == row % blocks
    arrive.wait()
    labels = labels_here[...]
    wide = jnp.dot(jnp.broadcast_to(labels, (16, clients)).astype(jnp.bfloat16), spread,
                   preferred_element_type=jnp.float32)[0:1].astype(jnp.int32)
    pick = ((wide == row // blocks) & same_row).astype(jnp.bfloat16)

    hits = (labels == lax.broadcasted_iota(jnp.int32, (CLUSTERS, clients), 0)).astype(jnp.float32)
    counts = jnp.sum(hits, axis=1, keepdims=True)
    lane = lax.broadcasted_iota(jnp.int32, (CLUSTERS, LANES), 1)
    for tile in range(tail // CLUSTERS):
        table = jnp.where(lane + tile * LANES == me, counts, 0.0)
        at = other.shape[0] - tail + tile * CLUSTERS
        other[at:at + CLUSTERS, :] = table
        mine[at:at + CLUSTERS, :] = table

    for part in range(4):
        copies[2 * part].wait()
        copies[2 * part + 1].wait()
        sums = jnp.dot(pick, held[part].reshape(depth, columns), preferred_element_type=jnp.float32)
        target = other if part < 2 else mine
        for block in range(columns // LANES):
            to = (part % 2 * columns // LANES + block) * rows
            target[to:to + rows, :] = sums[:, block * LANES:(block + 1) * LANES]


def local_sums(tail, chain, where, deltas, labels_row):
    clients, blocks, width = deltas.shape
    columns = width // (8 * CHAINS)
    height = 4 * columns // LANES * CLUSTERS * blocks + tail
    out = pltpu.VMEM((height, LANES), jnp.float32)
    return pl.pallas_call(
        functools.partial(local_sums_kernel, tail, chain),
        out_shape=(out, out),
        in_specs=[SMEM, HBM, HBM],
        out_specs=(VMEM, VMEM),
        scratch_shapes=[
            pltpu.VMEM((4, clients, blocks, 2 * columns), jnp.bfloat16), pltpu.VMEM((1, clients), jnp.int32),
            pltpu.SemaphoreType.DMA((9,))],
        compiler_params=pltpu.CompilerParams(vmem_limit_bytes=16 << 20),
        name="local_sums",
    )(where, far_off(deltas), far_off(labels_row))


def split_kernel(tail, step, where, kept, arrived, send, keep):
    half = (kept.shape[0] - tail) // 2
    bit = bit_at(where[0], role_of(where[0]), step)
    for target, which in ((send, 1 - bit), (keep, bit)):
        rows = pl.ds(pl.multiple_of(which * half, CLUSTERS), half)
        target[0:half, :] = kept[rows, :] + arrived[rows, :]
        if tail:
            target[half:half + tail, :] = kept[2 * half:2 * half + tail, :] + arrived[2 * half:2 * half + tail, :]


def split(tail, step, where, kept, arrived):
    half = (kept.shape[0] - tail) // 2
    out = pltpu.VMEM((half + tail, LANES), jnp.float32)
    return pl.pallas_call(
        functools.partial(split_kernel, tail, step),
        out_shape=(out, out),
        in_specs=[SMEM, VMEM, VMEM],
        out_specs=(VMEM, VMEM),
        compiler_params=pltpu.CompilerParams(vmem_limit_bytes=8 << 20),
        name="split",
    )(where, near(kept), near(arrived))


def table_of(tail, kept, arrived):
    ends = [kept.shape[0] - tail + at for at in range(0, tail, CLUSTERS)]
    return [kept[at:at + CLUSTERS, :] + arrived[at:at + CLUSTERS, :] for at in ends]


def finish_kernel(tail, own_tail, blocks, table, table_arrived, kept, arrived, models):
    rows = CLUSTERS * blocks
    height = kept.shape[0] - own_tail
    totals = jnp.zeros((CLUSTERS, 1), jnp.float32)
    for counts in table_of(tail, table, table_arrived):
        totals = totals + jnp.sum(counts, axis=1, keepdims=True)
    for cluster in range(CLUSTERS):
        total = jnp.broadcast_to(totals[cluster:cluster + 1, :], (blocks, LANES))
        for block in range(height // rows):
            at = block * rows + cluster * blocks
            sums = kept[at:at + blocks, :] + arrived[at:at + blocks, :]
            models[cluster * blocks:(cluster + 1) * blocks, block * LANES:(block + 1) * LANES] = (
                sums / total).astype(jnp.bfloat16)


def finish(tail, own_tail, blocks, table, kept, arrived):
    rows = CLUSTERS * blocks
    columns = (kept.shape[0] - own_tail) // rows * LANES
    return pl.pallas_call(
        functools.partial(finish_kernel, tail, own_tail, blocks),
        out_shape=pltpu.VMEM((rows, columns), jnp.bfloat16),
        in_specs=[VMEM] * 4,
        out_specs=VMEM,
        compiler_params=pltpu.CompilerParams(vmem_limit_bytes=8 << 20),
        name="finish",
    )(near(table[0]), near(table[1]), near(kept), near(arrived))


def join_kernel(*refs):
    at = 0
    for part in refs[:-1]:
        refs[-1][at:at + part.shape[0]] = part[...]
        at += part.shape[0]


def join(*parts):
    slots = sum(part.shape[0] for part in parts)
    return pl.pallas_call(
        join_kernel,
        out_shape=pltpu.VMEM((slots,) + parts[0].shape[1:], parts[0].dtype),
        in_specs=[VMEM] * len(parts),
        out_specs=VMEM,
        compiler_params=pltpu.CompilerParams(vmem_limit_bytes=8 << 20),
        name="join",
    )(*[near(part) for part in parts])


def ranks_of(me, table, labels):
    clients = labels.shape[1]
    lane = lax.broadcasted_iota(jnp.int32, (CLUSTERS, LANES), 1)
    before = jnp.zeros((CLUSTERS, 1), jnp.float32)
    for tile, counts in enumerate(table):
        before = before + jnp.sum(jnp.where(lane + tile * LANES < me, counts, 0.0), axis=1, keepdims=True)
    hits = labels == lax.broadcasted_iota(jnp.int32, (CLUSTERS, clients), 0)
    earlier = (lax.broadcasted_iota(jnp.int32, (clients, clients), 0)
               < lax.broadcasted_iota(jnp.int32, (clients, clients), 1))
    local = jnp.dot(hits.astype(jnp.float32).astype(jnp.bfloat16), earlier.astype(jnp.float32).astype(jnp.bfloat16),
                    preferred_element_type=jnp.float32)
    return jnp.sum(jnp.where(hits, before + local, 0.0), axis=0, keepdims=True).astype(jnp.int32)


def early_places(me):
    role = role_of(me)
    return [
        (quarter_of(me), [(chain, other, chain, role ^ other) for chain in range(CHAINS) for other in range(2)]),
        (quarter_of(me ^ (2 << role)), [(CHAINS, 1, 0, role), (CHAINS, 2, 0, 1 - role)]),
        (quarter_of(me ^ 6), [(CHAINS, 0, 0, role)]),
    ]


def late_places(me):
    role = role_of(me)
    return [
        (quarter_of(me ^ (4 >> role)), [
            (2 * chain, slot, chain, role ^ other) for chain in range(CHAINS) for slot, other in ((1, 1), (2, 0))]),
        (quarter_of(me ^ (2 << role)), [(1, 1, 1, role), (1, 2, 1, 1 - role)]),
        (quarter_of(me ^ 6), [(1, 0, 1, role), (2, 0, 1, 1 - role)]),
        (quarter_of(me ^ 6), [(0, 0, 0, 1 - role)]),
    ]


def give_back_kernel(places, arrays, tail, where, labels, *rest):
    me = where[0]
    models, rest = rest[:arrays], rest[arrays:]
    if tail:
        kept, arrived, labels_row, returned, rank, laid, sem, rank_here, rank_sem = rest
    else:
        _, returned, laid, sem = rest
    columns = models[0].shape[2]
    clients, blocks, _ = returned.shape
    ends, offset = [], 0
    for at, (quarter, pieces) in enumerate(places(me)):
        size = len(pieces) * columns
        first = pieces[0][2] * 2 + (pieces[0][3] if len(pieces) == 1 else 0)
        for array, slot, chain, half in pieces:
            to = offset + (chain * 2 + half - first) * columns
            to = pl.ds(pl.multiple_of(to, LANES), columns)
            for cluster in range(CLUSTERS):
                laid[cluster, :, to] = models[array][slot, cluster * blocks:(cluster + 1) * blocks, :]
        across = pl.ds(pl.multiple_of((quarter * CHAINS * 2 + first) * columns, LANES), size)
        for client in range(clients):
            pltpu.make_async_copy(
                laid.at[labels[client], :, offset:offset + size], returned.at[client, :, across], sem.at[at]).start()
        whole = returned.at[:, :, across]
        ends.append(pltpu.make_async_copy(whole, whole, sem.at[at]))
        offset += size
    if tail:
        rank_here[...] = ranks_of(me, table_of(tail, kept, arrived), labels_row[...])
        ends.append(pltpu.make_async_copy(rank_here, rank, rank_sem))
        ends[-1].start()
    for end in ends:
        end.wait()


def give_back(places, where, labels, models, shape, returned=None, ranked=None):
    columns = models[0].shape[2]
    slots = sum(array.shape[0] for array in models)
    scratch = [pltpu.VMEM((CLUSTERS, shape[1], slots * columns), jnp.bfloat16), pltpu.SemaphoreType.DMA((4,))]
    out = [jax.ShapeDtypeStruct(shape, jnp.bfloat16)]
    if ranked is None:
        tail, more, more_specs, aliases = 0, (returned,), [ANY], {2 + len(models): 0}
    else:
        tail, kept, arrived, labels_row = ranked
        more, more_specs, aliases = (near(kept), near(arrived), near(labels_row)), [VMEM] * 3, {}
        out.append(jax.ShapeDtypeStruct(labels_row.shape, jnp.int32))
        scratch += [pltpu.VMEM(labels_row.shape, jnp.int32), pltpu.SemaphoreType.DMA]
    return pl.pallas_call(
        functools.partial(give_back_kernel, places, len(models), tail),
        out_shape=out,
        in_specs=[SMEM, SMEM] + [VMEM] * len(models) + more_specs,
        out_specs=[ANY] * len(out),
        scratch_shapes=scratch,
        input_output_aliases=aliases,
        compiler_params=pltpu.CompilerParams(vmem_limit_bytes=8 << 20),
        cost_estimate=pl.CostEstimate(flops=COVER, bytes_accessed=0, transcendentals=0),
        name="give_back",
    )(where, labels, *[near(array) for array in models], *more)


def on_device(devices, deltas, labels):
    clients, blocks, _ = deltas.shape
    where = lax.axis_index(AXES).astype(jnp.int32).reshape(1)
    labels_row = labels.reshape(1, clients)
    labels_list = labels.reshape(clients)
    tail = count_rows(devices)
    tails = [0 if chain else tail for chain in range(CHAINS)]
    bits = devices.bit_length() - 1

    def send(value, flip):
        return lax.ppermute(value, AXES, [(i, i ^ flip(i)) for i in range(devices)])

    def cores(i):
        return 1

    def crossed(low, high, step):
        def flip(i):
            return 1 << (high - 1 - step if role_of(i) else low + step) | 1

        return flip

    kept = []
    for chain in range(CHAINS):
        other, mine = local_sums(tails[chain], chain, where, deltas, labels_row)
        kept.append(split(tails[chain], 0, where, mine, send(other, cores)))
    for chain, (out, keep) in enumerate(kept):
        kept[chain] = split(tails[chain], 1, where, keep, send(out, crossed(1, 3, 0)))
    for chain, (out, keep) in enumerate(kept):
        kept[chain] = (keep, send(out, crossed(1, 3, 1)))
    for step in range(bits - 3):
        for chain, (keep, arrived) in enumerate(kept):
            total = keep + arrived
            kept[chain] = (total, send(total, crossed(3, bits, step)))
    pairs, rests = [], []
    for chain, pair in enumerate(kept):
        own = finish(tail, tails[chain], blocks, kept[0], *pair)[None]
        diagonal = send(own, lambda i: 6)
        pairs.append(join(own, send(own, cores)))
        beside = send(pairs[-1], lambda i: 2 << role_of(i) | 1)
        taken = join(diagonal, beside)
        rests.append([taken, send(taken, cores)])

    give = functools.partial(give_back, where=where, labels=labels_list, shape=deltas.shape)
    returned, rank = give(early_places, models=pairs + rests[0][:1], ranked=(tail, *kept[0], labels_row))
    returned, = give(late_places, models=rests[0][1:] + rests[1], returned=returned)
    return returned, rank.reshape(clients)


def solution(mesh):
    devices = mesh.shape["dp"] * mesh.shape["group"]
    placed = (P(AXES, None, None), P(AXES, None))

    def body(deltas, labels):
        return on_device(devices, deltas, labels)

    return jax.shard_map(
        body,
        mesh=mesh,
        in_specs=placed,
        out_specs=(P(AXES, None, None), P(AXES)),
        check_vma=False,
    )
```
